32 devices in a mesh: grp: 2 (over y), seq: 16 (over z, x, core).
Axes of the slice: x: 2, y: 2, z: 4, core: 2. Of those that a mesh axis runs over, the one named last changes fastest.
Arguments:
- history: bfloat16 [8192, 1024], P(('grp', 'seq')), parts along dimension 0, may hold values from -6 to 6
- candidates: bfloat16 [512, 1024], P(('grp', 'seq')), parts along dimension 0, may hold values from -6 to 6
- lengths: int32 [8], P('grp'), parts along dimension 0, may hold values from 1 to 2048, 4096 in all
- cand_user: int32 [512], P(('grp', 'seq')), parts along dimension 0, may hold values from 0 to 3
- w_in: bfloat16 [1, 1024, 4096], replicated, may hold values from -0.125 to 0.125
- w_out: bfloat16 [1, 1024, 1024], replicated, may hold values from -0.1875 to 0.1875
Outputs:
- history_out: bfloat16 [8192, 1024], P(('grp', 'seq')), parts along dimension 0
- cand_out: bfloat16 [512, 1024], P(('grp', 'seq')), parts along dimension 0
The draws below stay inside these ranges and needn't reach their ends.
There are 2 independent parts, one for each index of `grp`. The reference program is written for one: setup_inputs(seed, part) draws one part's arguments, and reference() takes and returns one part's arrays. A program takes and returns all parts, laid end to end along the dimension named above; an argument that names none is the same for every part. Nothing has to cross between parts.
Inputs may be any that keep to these rules, and one draw needn't show every extreme that they name: Each user's history length is at least 1; the lengths sum to 4096, and one of them is exactly 2048.
All inputs are finite; a program needn't handle non-finite values.
Results may differ from the reference program's by a relative error of at most 0.0075.
Values may be sent and summed in bfloat16 or wider, within the bound.
A program may use at most 128 MiB of HBM per device.

```python
import math
import jax
import jax.numpy as jnp
import numpy as np
from jax import lax

D = 1024
HEADS = 8
HEAD_DIM = 128
LAYERS = 1
TOK_DEV = 256
HIST = 4096
WIN = 8
SPAN = 1792
USERS = 4
MOSTLEN = 2048
CANDS = 256
N_SEQ = 16


def draw_w_in(key, part):
    noise_key = jax.random.fold_in(key, 11)
    head_key = jax.random.fold_in(key, 23)
    independent = jax.random.normal(noise_key, (LAYERS, D, 4 * D), jnp.float32)
    weight_share = 0.7
    common = jax.random.normal(head_key, (LAYERS, D, 2, HEADS, 1), jnp.float32)
    common = jnp.broadcast_to(common, (LAYERS, D, 2, HEADS, D // HEADS)).reshape(LAYERS, D, 2 * D)
    query_key = weight_share * common + (1.0 - weight_share * weight_share) ** 0.5 * independent[:, :, 2 * D:]
    complete = jnp.concatenate([independent[:, :, 0:2 * D], query_key], axis=2)
    return (jnp.clip(complete, -4.0, 4.0) * D ** (-0.5)).astype(jnp.bfloat16)


def with_ends(drawn, key, low, high):
    dims = drawn.shape
    spot = [jax.random.randint(jax.random.fold_in(key, axis), (), 0, dims[axis]) for axis in range(len(dims))]
    drawn = drawn.at[tuple(spot)].set(low)
    longest = dims.index(max(dims))
    spot[longest] = (spot[longest] + 1) % dims[longest]
    return drawn.at[tuple(spot)].set(high)


def block_levels(rng, extent, cuts, low, high):
    def one(axis_at, parts):
        steps = jax.random.uniform(jax.random.fold_in(jax.random.fold_in(rng, 6), axis_at), (parts,), jnp.float32, low / len(cuts), high / len(cuts))
        return jnp.repeat(jnp.exp(steps), extent[axis_at] // parts).reshape((-1,) + (1,) * (len(extent) - axis_at - 1))

    level = one(*cuts[0])
    for cut in cuts[1:]:
        level = level * one(*cut)
    return level


def profile(number_of, total, reach, skew):
    portions = [(1 << 20) // math.isqrt(standing ** skew) + 1 for standing in range(2, number_of + 1)]
    surplus, counts = total - reach - (number_of - 1), [1] * (number_of - 1)
    while surplus > 0:
        free = [i for i in range(number_of - 1) if counts[i] < reach]
        pool, left = sum([portions[i] for i in free]), surplus
        for i in free:
            addition = min(reach - counts[i], max(1, left * portions[i] // pool), surplus)
            counts[i] = counts[i] + addition
            surplus = surplus - addition
    return np.array([reach] + counts)


def ragged(rng, amount, total, most, lean):
    if amount == 2:
        one = jax.random.randint(rng, (), max(1, total - most), min(most, total - 1) + 1)
        return jnp.stack([one, total - one])
    sizes = jnp.asarray(profile(amount, total, most, lean), jnp.int32)
    couples = (amount - 1) // 2
    donor, receiver = sizes[1:1 + 2 * couples:2], sizes[2:2 + 2 * couples:2]
    slack = jnp.minimum(donor - 1, most - receiver)
    passed = jax.random.randint(jax.random.fold_in(rng, 1), (couples,), 0, 1 << 20) % (slack + 1)
    sizes = sizes.at[1:1 + 2 * couples:2].set(donor - passed).at[2:2 + 2 * couples:2].set(receiver + passed)
    return sizes[jax.random.permutation(jax.random.fold_in(rng, 2), amount)]


def noise(stream_key, dims, deviation, reach, split=(), kind=jnp.bfloat16):
    loudness = block_levels(stream_key, dims, split, -0.22, 0.18) if split else 1.0
    array = jax.random.normal(stream_key, dims, jnp.float32) * deviation * loudness
    return jnp.minimum(jnp.maximum(array, -reach), reach).astype(kind)


def setup_inputs(seed: int = 0, part: int = 0) -> dict:
    key_list = jax.random.split(jax.random.key(seed), 7)
    own_keys = jax.random.split(jax.random.fold_in(key_list[6], part), 7)
    history = noise(own_keys[0], (HIST, D), 1.0, 6.0, ((0, 16),))
    candidates = noise(own_keys[1], (CANDS, D), 1.0, 6.0, ((0, 16),))
    lengths = ragged(own_keys[2], USERS, HIST, MOSTLEN, 2).astype(jnp.int32)
    cand_user = with_ends(jax.random.randint(own_keys[3], (CANDS,), 0, USERS), jax.random.fold_in(own_keys[3], 1), 0, USERS - 1).astype(jnp.int32)
    w_in = draw_w_in(jax.random.fold_in(key_list[6], 71), part)
    w_out = noise(key_list[5], (LAYERS, D, D), D ** -0.5, 0.1875)
    return {"history": history, "candidates": candidates, "lengths": lengths, "cand_user": cand_user, "w_in": w_in, "w_out": w_out}


eps = 1e-06

def layer_norm(rows):
    centred = rows - lax.optimization_barrier(jnp.mean(rows, axis=-1, keepdims=True))
    return centred * lax.rsqrt(lax.optimization_barrier(jnp.mean(centred * centred, axis=-1, keepdims=True)) + eps)

def segment_of(positions, ends):
    return lax.optimization_barrier(jnp.sum((positions[:, None] >= ends[None, :]).astype(jnp.int32), axis=1)).astype(jnp.int32)

def reference(history, candidates, lengths, cand_user, w_in, w_out):
    ends = jnp.cumsum(lengths).astype(jnp.int32)
    scale = HEAD_DIM ** (-0.5)
    width = WIN * TOK_DEV
    x_rows = history
    c_rows = candidates
    all_seg = segment_of(jnp.arange(HIST, dtype=jnp.int32), ends)
    for layer in range(LAYERS):
        normed = layer_norm(x_rows.astype(jnp.float32)).astype(jnp.bfloat16)
        proj = jax.nn.silu(jnp.dot(normed, w_in[layer], preferred_element_type=jnp.float32)).astype(jnp.bfloat16)
        u_all = proj[:, 0:D]
        v_all = proj[:, D:2 * D]
        q_all = proj[:, 2 * D:3 * D]
        k_all = proj[:, 3 * D:4 * D]
        front = jnp.zeros(((WIN - 1) * TOK_DEV, D), jnp.bfloat16)
        k_pad = jnp.concatenate([front, k_all], axis=0)
        v_pad = jnp.concatenate([front, v_all], axis=0)

        def hist_block(block):
            first = (block * TOK_DEV).astype(jnp.int32)
            q_blk = lax.dynamic_slice_in_dim(q_all, first, TOK_DEV, 0).astype(jnp.float32).reshape(TOK_DEV, HEADS, HEAD_DIM)
            k_blk = lax.dynamic_slice_in_dim(k_pad, first, width, 0).astype(jnp.float32).reshape(width, HEADS, HEAD_DIM)
            v_blk = lax.dynamic_slice_in_dim(v_pad, first, width, 0).astype(jnp.float32).reshape(width, HEADS, HEAD_DIM)
            q_pos = first + jnp.arange(TOK_DEV, dtype=jnp.int32)
            k_pos = first - (WIN - 1) * TOK_DEV + jnp.arange(width, dtype=jnp.int32)
            allowed = (k_pos[None, :] >= 0) & (k_pos[None, :] <= q_pos[:, None])
            allowed = allowed & (q_pos[:, None] - k_pos[None, :] < SPAN)
            allowed = allowed & (segment_of(k_pos, ends)[None, :] == segment_of(q_pos, ends)[:, None])
            scores = jnp.einsum('qhd,khd->hqk', q_blk, k_blk) * scale
            weight = jnp.where(allowed[None], jax.nn.silu(scores), 0.0).astype(jnp.bfloat16)
            return jnp.einsum('hqk,khd->qhd', weight.astype(jnp.float32), v_blk).reshape(TOK_DEV, D)
        attn = lax.map(hist_block, jnp.arange(N_SEQ, dtype=jnp.int32)).reshape(HIST, D)
        y_rows = (layer_norm(attn) * u_all.astype(jnp.float32)).astype(jnp.bfloat16)
        x_rows = (x_rows.astype(jnp.float32) + jnp.dot(y_rows, w_out[layer], preferred_element_type=jnp.float32)).astype(jnp.bfloat16)
        cnormed = layer_norm(c_rows.astype(jnp.float32)).astype(jnp.bfloat16)
        u_c = jax.nn.silu(jnp.dot(cnormed, w_in[layer][:, 0:D], preferred_element_type=jnp.float32)).astype(jnp.bfloat16)
        q_c = jax.nn.silu(jnp.dot(cnormed, w_in[layer][:, 2 * D:3 * D], preferred_element_type=jnp.float32)).astype(jnp.bfloat16)
        cq_heads = q_c.astype(jnp.float32).reshape(CANDS, HEADS, HEAD_DIM)

        def cand_shard(block, total):
            first = (block * TOK_DEV).astype(jnp.int32)
            k_blk = lax.dynamic_slice_in_dim(k_all, first, TOK_DEV, 0).astype(jnp.float32).reshape(TOK_DEV, HEADS, HEAD_DIM)
            v_blk = lax.dynamic_slice_in_dim(v_all, first, TOK_DEV, 0).astype(jnp.float32).reshape(TOK_DEV, HEADS, HEAD_DIM)
            k_seg = lax.dynamic_slice_in_dim(all_seg, first, TOK_DEV, 0)
            owned = cand_user[:, None] == k_seg[None, :]
            scores = jnp.einsum('chd,khd->hck', cq_heads, k_blk) * scale
            weight = jnp.where(owned[None], jax.nn.silu(scores), 0.0).astype(jnp.bfloat16)
            return total + jnp.einsum('hck,khd->chd', weight.astype(jnp.float32), v_blk).reshape(CANDS, D)
        cattn = lax.fori_loop(0, N_SEQ, cand_shard, jnp.zeros((CANDS, D), jnp.float32))
        y_c = (layer_norm(cattn) * u_c.astype(jnp.float32)).astype(jnp.bfloat16)
        c_rows = (c_rows.astype(jnp.float32) + jnp.dot(y_c, w_out[layer], preferred_element_type=jnp.float32)).astype(jnp.bfloat16)
    return (x_rows, c_rows)
```

```python
import functools

import jax
import jax.numpy as jnp
from jax import lax
from jax.experimental import pallas as pl
from jax.experimental.pallas import tpu as pltpu
from jax.sharding import PartitionSpec as P

HEADS = 8
WIN = 8
PIECES = 4
ROW = 4
SIB = 6
B1, B2, B3, B4, B5 = 0, 1, 2, 3, 4

eps = 1e-06
bf16 = jnp.bfloat16
f32 = jnp.float32


def layer_norm(rows):
    centred = rows - jnp.mean(rows, axis=-1, keepdims=True)
    return centred * lax.rsqrt(jnp.mean(centred * centred, axis=-1, keepdims=True) + eps)


def silu_of_twice(half):
    return half + half * jnp.tanh(half)


def dot(a, b):
    return jnp.dot(a, b, preferred_element_type=f32)


def dot_t(a, b):
    return lax.dot_general(a, b, (((1,), (1,)), ((), ())), preferred_element_type=f32)


def pick(i, entries):
    out = 0
    for at, value in entries.items():
        out = out + value * (1 - jnp.minimum((i - at) * (i - at), 1))
    return out


def kernel(
    n,
    lengths,
    hist,
    cand,
    users_row,
    w_in_hbm,
    w_out_hbm,
    out_ref,
    cout_ref,
    w_in,
    w_out,
    own,
    xb,
    kv,
    q_s,
    u_s,
    acc,
    cmsg,
    cbuf,
    qc_s,
    part,
    buf1,
    out3,
    buf3,
    fin,
    cfin,
    w_sem,
    x_send,
    x_recv,
    kv_send,
    kv_recv,
    c_send,
    c_recv,
    up_send,
    down_send,
    rz_send,
    rz_recv,
):
    rows, width = hist.shape
    cr = cand.shape[0]
    head_dim = width // HEADS
    half_scale = 0.5 * head_dim ** (-0.5)
    depth = n // ROW
    s = lax.axis_index("seq")
    z = s // ROW
    r = s % ROW
    p = r // 2
    k = r % 2
    piece = rows // PIECES
    sibling = s + 1 - 2 * k
    partner = s + 2 - 4 * p
    above = (s + ROW) % n
    below = (s + n - ROW) % n
    has_above = z + 1 < depth
    has_below = z >= 1

    w_copies = [
        pltpu.make_async_copy(
            w_in_hbm.at[0, :, pl.ds(c * width, width)], w_in.at[c], w_sem.at[c]
        )
        for c in range(4)
    ]
    w_copies.append(pltpu.make_async_copy(w_out_hbm.at[0], w_out, w_sem.at[4]))
    for c in (3, 1, 2, 0, 4):
        w_copies[c].start()

    barrier = pltpu.get_barrier_semaphore()

    def greet(to):
        pl.semaphore_signal(barrier, inc=1, device_id={"seq": to}, device_id_type=pl.DeviceIdType.MESH)

    peers = (
        (None, sibling),
        (None, partner),
        (has_above, above),
        (has_below, below),
        (has_above & (k == 1), (s + 3) % n),
        (has_below & (k == 0), (s + n - 3) % n),
        (r == 1, (s + 1) % n),
        (r == 2, (s + n - 1) % n),
    )
    for cond, to in peers:
        if cond is None:
            greet(to)
        else:
            pl.when(cond)(functools.partial(greet, to))

    eye = lax.broadcasted_iota(jnp.int32, (cr, cr), 0) == lax.broadcasted_iota(jnp.int32, (cr, cr), 1)
    column = jnp.sum(jnp.where(eye, users_row[...], 0), axis=1, keepdims=True)
    c_normed = layer_norm(cand[...].astype(f32)).astype(bf16)
    cmsg[:, :width] = c_normed
    cmsg[:, width:] = jnp.broadcast_to(column, (cr, 128)).astype(f32).astype(bf16)

    @pl.when(p == 1)
    def _():
        cbuf[k, z, pl.ds(cr, cr)] = cmsg[...]

    normed = layer_norm(hist[...].astype(f32)).astype(bf16)
    own[...] = normed
    pl.semaphore_wait(barrier, sum(1 if cond is None else cond.astype(jnp.int32) for cond, _ in peers))

    def remote(src, dst, send, recv, to):
        return pltpu.make_async_remote_copy(
            src_ref=src,
            dst_ref=dst,
            send_sem=send,
            recv_sem=recv,
            device_id={"seq": to},
            device_id_type=pl.DeviceIdType.MESH,
        )

    def x_copy(src, dst, h, kind, to):
        at = pl.ds(h * piece, piece)
        return remote(src.at[at], xb.at[dst, at], x_send.at[kind, h], x_recv.at[dst, h], to)

    moves = (
        (0, own, B2, above, has_above, None),
        (1, own, B1, partner, p == 0, None),
        (2, xb.at[B2], B3, partner, has_below, B2),
        (3, xb.at[B2], B5, (s + 3) % n, has_below & has_above & (k == 1), B2),
        (4, xb.at[B3], B4, above, has_below & has_above & (r == 0), B3),
        (5, xb.at[B5], B4, (s + n - 1) % n, (z >= 2) & (r == 2), B5),
    )
    arrives = {
        B1: p == 1,
        B2: has_below,
        B3: has_below,
        B4: (z >= 2) & (p == 0),
        B5: (z >= 2) & (k == 0),
    }

    def c_cross():
        return remote(cmsg, cbuf.at[k, z, pl.ds(0, cr)], c_send.at[0], c_recv.at[depth], partner)

    def c_block(block, send, to):
        return remote(cbuf.at[k, block], cbuf.at[k, block], send, c_recv.at[block], to)

    def c_swap():
        return remote(cbuf.at[k], cbuf.at[k], c_send.at[1], c_recv.at[depth + 1], sibling)

    @pl.when(p == 0)
    def _():
        c_cross().start()

    for h in range(PIECES):
        for kind, src, dst, to, cond, _ in moves[:2]:

            @pl.when(cond)
            def _():
                x_copy(src, dst, h, kind, to).start()

    def hop(buf, h):
        at = pl.ds(h * piece, piece)

        @pl.when(arrives[buf])
        def _():
            pltpu.make_async_copy(hist.at[at], xb.at[buf, at], x_recv.at[buf, h]).wait()
            for kind, src, dst, to, cond, source in moves:
                if source == buf:

                    @pl.when(cond)
                    def _():
                        x_copy(src, dst, h, kind, to).start()

    ends = []
    total = jnp.int32(0)
    for j in range(lengths.shape[0]):
        total = total + lengths[j]
        ends.append(total)

    def seg(pos):
        out = jnp.zeros(pos.shape, jnp.int32)
        for e in ends:
            out = out + (pos >= e).astype(jnp.int32)
        return out

    q_pos = s * rows + lax.broadcasted_iota(jnp.int32, (rows, 1), 0)
    q_seg = seg(q_pos)

    def project(normed, block):
        return silu_of_twice(dot(normed, w_in[block]) * 0.5).astype(bf16)

    def swap_copy(t):
        return remote(kv.at[t], kv.at[SIB + t], kv_send.at[t], kv_recv.at[t], sibling)

    def shard_of(t, kk):
        ahead = pick(t, {1: ROW * z + kk, 2: ROW * (z - 1) + 2 * p + kk, 3: ROW * (z - 1) + 2 - 2 * p + kk})
        return ahead + pick(t, {0: ROW * z + 2 * p + kk, 4: ROW * (z - 2) + 2 + kk, 5: ROW * (z - 2) + 1 + 2 * p})

    def attend(a):
        side = a // SIB
        t = a % SIB
        shard = shard_of(t, k + side - 2 * k * side)
        k_pos = shard * rows + lax.broadcasted_iota(jnp.int32, (1, rows), 1)
        ok = (k_pos <= q_pos) & (q_pos - k_pos < (WIN - 1) * rows) & (seg(k_pos) == q_seg)
        for h in range(HEADS):
            cols = slice(h * head_dim, (h + 1) * head_dim)
            half = dot_t(q_s[:, cols], kv[a, 0, :, cols]) * half_scale
            weight = jnp.where(ok, silu_of_twice(half), 0.0).astype(bf16)
            acc[:, cols] += dot(weight, kv[a, 1, :, cols])

    w_copies[3].wait()
    kv[0, 0] = project(normed, 3)
    w_copies[1].wait()
    kv[0, 1] = project(normed, 1)

    @pl.when(k == 0)
    def _():
        swap_copy(0).start()

    def c_round(d):
        low = jnp.maximum(z - d, 0)
        high = jnp.minimum(z + d, depth - 1)
        if isinstance(d, int) and d == 0:
            pl.when(has_above)(lambda: c_block(z, up_send.at[d], above).start())
            pl.when(has_below)(lambda: c_block(z, down_send.at[d], below).start())
            return

        @pl.when(z - d >= 0)
        def _():
            c_block(low, up_send.at[d], above).wait_recv()
            pl.when(has_above)(lambda: c_block(low, up_send.at[d], above).start())

        @pl.when(z + d < depth)
        def _():
            c_block(high, down_send.at[d], below).wait_recv()
            pl.when(has_below)(lambda: c_block(high, down_send.at[d], below).start())

    def c_first():
        remote(cmsg, cbuf.at[k, z, pl.ds(0, cr)], c_send.at[0], c_recv.at[depth], partner).wait_recv()
        c_round(0)

    pl.when(p == 1)(c_first)
    w_copies[2].wait()
    q_s[...] = project(normed, 2)
    w_copies[0].wait()
    u_s[...] = project(jnp.concatenate([normed, c_normed], axis=0), 0)
    acc[...] = jnp.zeros_like(acc)
    if depth > 1:
        pl.when(p == 1)(functools.partial(c_round, 1))

    block_rows = part.shape[1]
    k_seg = seg(s * rows + lax.broadcasted_iota(jnp.int32, (1, rows), 1)).astype(f32)
    kk_seg = seg((ROW * z + k) * rows + lax.broadcasted_iota(jnp.int32, (1, rows), 1)).astype(f32)
    group = qc_s.shape[1]
    groups = 2 * block_rows // group
    lines = group // (2 * cr)

    def c_queries():
        def one(b, carry):
            if groups == 1:
                x = cbuf[:, :, :, :width].reshape(group, width)
            else:
                per = groups // 2
                x = cbuf[b // per, pl.ds(b % per * lines, lines), :, :width].reshape(group, width)
            qc_s[b] = project(x, 2)
            return carry

        lax.fori_loop(0, groups, one, 0)

    def c_attend(t, segs):
        def one(b, carry):
            per = max(groups // 2, 1)
            if groups == 1:
                owner = cbuf[:, :, :, width:].reshape(group, 128)[:, :1]
            else:
                owner = cbuf[b // per, pl.ds(b % per * lines, lines), :, width:].reshape(group, 128)[:, :1]
            ok = owner.astype(f32) == segs
            for h in range(HEADS):
                cols = slice(h * head_dim, (h + 1) * head_dim)
                half = dot_t(qc_s[b, :, cols], kv[t, 0, :, cols]) * half_scale
                weight = jnp.where(ok, silu_of_twice(half), 0.0).astype(bf16)
                value = dot(weight, kv[t, 1, :, cols])
                if groups == 1:
                    value = value.reshape(2, block_rows, head_dim)
                    if t:
                        value = value + part[:, :, cols]
                    part[:, :, cols] = value
                else:
                    at = pl.ds(pl.multiple_of(b % per * group, group), group)
                    if t:
                        value = value + part[b // per, at, cols]
                    part[b // per, at, cols] = value
            return carry

        lax.fori_loop(0, groups, one, 0)

    def red1():
        return remote(part.at[1 - k], buf1, c_send.at[2], c_recv.at[depth + 2], sibling)

    def red3(d):
        return remote(out3.at[(z + d) % depth], buf3.at[d], rz_send.at[d], rz_recv.at[d], (s + ROW * d) % n)

    def red4():
        return remote(fin, cfin, c_send.at[3], c_recv.at[depth + 3], partner)

    def c_middle():
        def rest(d, carry):
            c_round(d)
            return carry

        lax.fori_loop(3, depth, rest, 0)
        c_swap().start()
        c_swap().wait_recv()
        c_queries()
        c_attend(0, k_seg)

    def c_late():
        c_attend(1, kk_seg)
        red1().start()

    def c_sums():
        red1().wait_recv()
        part[k] += buf1[...]
        out3[...] = part[k].astype(bf16).reshape(out3.shape)

        def send(d, c):
            red3(d).start()
            return c

        lax.fori_loop(1, depth, send, 0)

    def c_done():
        mine = part[k, pl.ds(pl.multiple_of(z * 2 * cr, 2 * cr), 2 * cr)]

        def take(d, c):
            red3(d).wait_recv()
            return c + buf3[d].astype(f32)

        mine = lax.fori_loop(1, depth, take, mine)
        fin[...] = mine[:cr]
        red4().start()
        cfin[...] = mine[cr:]

    def event(e):
        if e == 1:
            hop(B2, 0)
            if depth > 2:
                pl.when(p == 1)(functools.partial(c_round, 2))
        if e == 2:
            hop(B2, 1)
            pl.when(p == 1)(c_middle)
            hop(B2, 2)
            hop(B2, 3)
            for h in range(PIECES):
                hop(B1, h)

            pl.when(p == 0)(functools.partial(hop, B3, 0))
            pl.when(p == 0)(functools.partial(hop, B3, 1))
        if e == 3:
            pl.when(p == 0)(functools.partial(hop, B3, 2))
            pl.when(p == 1)(functools.partial(hop, B5, 0))
        if e == 4:
            pl.when(p == 0)(functools.partial(hop, B3, 3))
            pl.when(p == 1)(functools.partial(hop, B5, 1))
            pl.when(p == 1)(functools.partial(hop, B5, 2))
        if e == 5:
            pl.when(p == 1)(functools.partial(hop, B5, 3))
            pl.when(p == 1)(c_late)
        if e == 6:
            pl.when(p == 1)(c_sums)
        if e == 7:
            for h in range(PIECES):
                pl.when(p == 0)(functools.partial(hop, B4, h))
        if e == 8:
            for h in range(PIECES):
                pl.when(p == 1)(functools.partial(hop, B3, h))
                pl.when(p == 0)(functools.partial(hop, B5, h))
        if e == 9:
            pl.when(p == 1)(c_done)

    proj_at = {2: (2, 1), 3: (0, 2), 5: (3, 0), 7: (4, 5), 8: (5, 3)}
    att_at = {
        0: (1, 1),
        1: (1 + SIB, 1 + SIB),
        3: (1 + 2, 1 + 1),
        4: (1 + SIB + 2, 1 + SIB + 1),
        5: (1 + 3, 1 + 2),
        6: (1 + SIB + 3, 1 + SIB + 2),
        7: (0, 1 + 5),
        8: (1 + 5, 1 + 3),
        9: (1 + 4, 1 + SIB + 3),
        10: (1 + SIB + 4, 0),
    }

    def mix(table):
        return {at: v0 * (1 - p) + v1 * p for at, (v0, v1) in table.items()}

    proj_table, att_table = mix(proj_at), mix(att_at)

    def one(e, carry):
        for at in range(11):

            @pl.when(e == at)
            def _():
                event(at)

        t = pick(e, proj_table)

        @pl.when((t > 0) & (z >= t // 2) & ((t < 5) | (k == 0)))
        def _():
            x = xb[t - jnp.minimum(t, 1)]
            kv[t, 0] = project(x, 3)
            kv[t, 1] = project(x, 1)
            pl.when(t < 5)(lambda: swap_copy(t).start())

        a = pick(e, att_table) - 1
        ta = (a + SIB) % SIB
        side = (a + SIB) // SIB - 1

        @pl.when((a >= 0) & (z >= ta // 2) & ((ta < 5) | (k == 0)) & ((ta > 0) | (side < 1) | (k == 1)))
        def _():
            pl.when(side == 1)(lambda: swap_copy(ta).wait_recv())
            attend(a)

        return carry

    lax.fori_loop(0, 11, one, 0)

    w_copies[4].wait()

    @pl.when(p == 0)
    def _():
        red4().wait_recv()

    y_c = (layer_norm(cfin[...]) * u_s[pl.ds(rows, cr)].astype(f32)).astype(bf16)
    y = (layer_norm(acc[...]) * u_s[pl.ds(0, rows)].astype(f32)).astype(bf16)
    both = dot(jnp.concatenate([y, y_c], axis=0), w_out[...])
    out_ref[...] = (hist[...].astype(f32) + both[:rows]).astype(bf16)
    cout_ref[...] = (cand[...].astype(f32) + both[rows:]).astype(bf16)

    for h in range(PIECES):
        for kind, src, dst, to, cond, _ in moves:

            @pl.when(cond)
            def _():
                x_copy(src, dst, h, kind, to).wait_send()

    for t, cond in ((0, k == 0), (1, p == 1), (2, z >= 1), (3, z >= 1), (4, (z >= 2) & (p == 0))):

        @pl.when(cond)
        def _():
            swap_copy(t).wait_send()

    pl.when(p == 0)(lambda: c_cross().wait_send())

    @pl.when(p == 1)
    def _():
        c_swap().wait_send()
        red1().wait_send()
        red4().wait_send()

        def left(d, c):
            pl.when(has_above & (z - d >= 0))(lambda: c_block(0, up_send.at[d], above).wait_send())
            pl.when(has_below & (z + d < depth))(lambda: c_block(0, down_send.at[d], below).wait_send())
            return c

        lax.fori_loop(0, depth, left, 0)

        def sums(d, c):
            red3(d).wait_send()
            return c

        lax.fori_loop(1, depth, sums, 0)


def per_device(n, history, candidates, lengths, cand_user, w_in, w_out):
    rows, width = history.shape
    cr = candidates.shape[0]
    depth = n // ROW
    users = cand_user[None, :]
    vmem = pl.BlockSpec(memory_space=pltpu.VMEM)
    dma = pltpu.SemaphoreType.DMA
    block = depth * 2 * cr
    group = 2 * block if 2 * block <= 256 else min(block, 256)
    return pl.pallas_call(
        functools.partial(kernel, n),
        out_shape=(
            jax.ShapeDtypeStruct((rows, width), bf16),
            jax.ShapeDtypeStruct((cr, width), bf16),
        ),
        in_specs=[
            pl.BlockSpec(memory_space=pltpu.SMEM),
            vmem,
            vmem,
            vmem,
            pl.BlockSpec(memory_space=pl.ANY),
            pl.BlockSpec(memory_space=pl.ANY),
        ],
        out_specs=(vmem, vmem),
        scratch_shapes=[
            pltpu.VMEM((4, width, width), bf16),
            pltpu.VMEM((width, width), bf16),
            pltpu.VMEM((rows, width), bf16),
            pltpu.VMEM((5, rows, width), bf16),
            pltpu.VMEM((SIB + 5, 2, rows, width), bf16),
            pltpu.VMEM((rows, width), bf16),
            pltpu.VMEM((rows + cr, width), bf16),
            pltpu.VMEM((rows, width), f32),
            pltpu.VMEM((cr, width + 128), bf16),
            pltpu.VMEM((2, depth, 2 * cr, width + 128), bf16),
            pltpu.VMEM((2 * block // group, group, width), bf16),
            pltpu.VMEM((2, block, width), f32),
            pltpu.VMEM((block, width), f32),
            pltpu.VMEM((depth, 2 * cr, width), bf16),
            pltpu.VMEM((depth, 2 * cr, width), bf16),
            pltpu.VMEM((cr, width), f32),
            pltpu.VMEM((cr, width), f32),
            dma((5,)),
            dma((6, PIECES)),
            dma((5, PIECES)),
            dma((5,)),
            dma((5,)),
            dma((4,)),
            dma((depth + 4,)),
            dma((depth,)),
            dma((depth,)),
            dma((depth,)),
            dma((depth,)),
        ],
        compiler_params=pltpu.CompilerParams(
            collective_id=0, has_side_effects=True, vmem_limit_bytes=60 * 1024 * 1024
        ),
    )(lengths, history, candidates, users, w_in, w_out)


def solution(mesh):
    n = mesh.shape["seq"]
    placed = (
        P(("grp", "seq"), None),
        P(("grp", "seq"), None),
        P("grp"),
        P(("grp", "seq")),
        P(),
        P(),
    )
    return jax.shard_map(
        functools.partial(per_device, n),
        mesh=mesh,
        in_specs=placed,
        out_specs=(P(("grp", "seq"), None), P(("grp", "seq"), None)),
        check_vma=False,
    )
```

```python
import functools

import jax
import jax.numpy as jnp
from jax import lax
from jax.experimental import pallas as pl
from jax.experimental.pallas import tpu as pltpu
from jax.sharding import PartitionSpec as P

HEADS = 8
WIN = 8
PIECES = 4
ROW = 4
EARLY = 3
SIB = 6
B1, B2, B3, B4, B5 = 0, 1, 2, 3, 4

eps = 1e-06
bf16 = jnp.bfloat16
f32 = jnp.float32


def layer_norm(rows):
    centred = rows - jnp.mean(rows, axis=-1, keepdims=True)
    return centred * lax.rsqrt(jnp.mean(centred * centred, axis=-1, keepdims=True) + eps)


def silu_of_twice(half):
    return half + half * jnp.tanh(half)


def dot(a, b):
    return jnp.dot(a, b, preferred_element_type=f32)


def dot_t(a, b):
    return lax.dot_general(a, b, (((1,), (1,)), ((), ())), preferred_element_type=f32)


def pick(i, entries):
    out = 0
    for at, value in entries.items():
        out = out + value * (1 - jnp.minimum((i - at) * (i - at), 1))
    return out


def kernel(
    n,
    lengths,
    hist,
    cand,
    users_row,
    w_in_hbm,
    w_out_hbm,
    out_ref,
    w_in,
    w_out,
    own,
    xb,
    kv,
    q_s,
    u_s,
    acc,
    cmsg,
    cbuf,
    qc_s,
    part,
    out3,
    buf3,
    w_sem,
    x_send,
    x_recv,
    kv_send,
    kv_recv,
    c_send,
    c_recv,
    up_send,
    down_send,
    rz_send,
    rz_recv,
):
    rows, width = hist.shape
    cr = cand.shape[0]
    head_dim = width // HEADS
    half_scale = 0.5 * head_dim ** (-0.5)
    depth = n // ROW
    s = lax.axis_index("seq")
    z = s // ROW
    r = s % ROW
    p = r // 2
    k = r % 2
    piece = rows // PIECES
    sibling = s + 1 - 2 * k
    partner = s + 2 - 4 * p
    above = (s + ROW) % n
    below = (s + n - ROW) % n
    has_above = z + 1 < depth
    has_below = z >= 1

    w_copies = [
        pltpu.make_async_copy(
            w_in_hbm.at[0, :, pl.ds(c * width, width)], w_in.at[c], w_sem.at[c]
        )
        for c in range(4)
    ]
    w_copies.append(pltpu.make_async_copy(w_out_hbm.at[0], w_out, w_sem.at[4]))
    for c in (3, 1, 2, 0, 4):
        w_copies[c].start()

    barrier = pltpu.get_barrier_semaphore()

    def greet(to):
        pl.semaphore_signal(barrier, inc=1, device_id={"seq": to}, device_id_type=pl.DeviceIdType.MESH)

    peers = (
        (None, sibling),
        (None, partner),
        (has_above, above),
        (has_below, below),
        (has_above & (k == 1), (s + 3) % n),
        (has_below & (k == 0), (s + n - 3) % n),
        (r == 1, (s + 1) % n),
        (r == 2, (s + n - 1) % n),
    )
    for cond, to in peers:
        if cond is None:
            greet(to)
        else:
            pl.when(cond)(functools.partial(greet, to))

    eye = lax.broadcasted_iota(jnp.int32, (cr, cr), 0) == lax.broadcasted_iota(jnp.int32, (cr, cr), 1)
    column = jnp.sum(jnp.where(eye, users_row[...], 0), axis=1, keepdims=True)
    c_normed = layer_norm(cand[...].astype(f32)).astype(bf16)
    cmsg[:, :width] = c_normed
    cmsg[:, width:] = jnp.broadcast_to(column, (cr, 128)).astype(f32).astype(bf16)

    @pl.when(p == 1)
    def _():
        cbuf[z, pl.ds(cr, cr)] = cmsg[...]

    normed = layer_norm(hist[...].astype(f32)).astype(bf16)
    own[...] = normed
    pl.semaphore_wait(barrier, sum(1 if cond is None else cond.astype(jnp.int32) for cond, _ in peers))

    def remote(src, dst, send, recv, to):
        return pltpu.make_async_remote_copy(
            src_ref=src,
            dst_ref=dst,
            send_sem=send,
            recv_sem=recv,
            device_id={"seq": to},
            device_id_type=pl.DeviceIdType.MESH,
        )

    def x_copy(src, dst, h, kind, to):
        at = pl.ds(h * piece, piece)
        return remote(src.at[at], xb.at[dst, at], x_send.at[kind, h], x_recv.at[dst, h], to)

    moves = (
        (0, own, B2, above, has_above, None),
        (1, own, B1, partner, p == 0, None),
        (2, xb.at[B2], B3, partner, has_below, B2),
        (3, xb.at[B2], B5, (s + 3) % n, has_below & has_above & (k == 1), None),
        (4, xb.at[B3], B4, above, has_below & has_above & (r == 0), B3),
        (5, xb.at[B5], B4, (s + n - 1) % n, (z >= 2) & (r == 2), B5),
    )
    arrives = {
        B1: p == 1,
        B2: has_below,
        B3: has_below,
        B4: (z >= 2) & (p == 0),
        B5: (z >= 2) & (k == 0),
    }

    def c_cross():
        return remote(cmsg, cbuf.at[z, pl.ds(0, cr)], c_send.at[0], c_recv.at[depth], partner)

    def c_block(block, send, to):
        return remote(cbuf.at[block], cbuf.at[block], send, c_recv.at[block], to)

    @pl.when(p == 0)
    def _():
        c_cross().start()

    def send(which, first, last, also=None):
        kind, src, dst, to, cond, _ = moves[which]

        @pl.when(cond if also is None else cond & also)
        def _():
            for h in range(first, last):
                x_copy(src, dst, h, kind, to).start()

    for h in range(PIECES):
        send(0, h, h + 1, None if h < EARLY else p == 0)
        send(1, h, h + 1)

    def hop(buf, h):
        at = pl.ds(h * piece, piece)

        @pl.when(arrives[buf])
        def _():
            pltpu.make_async_copy(hist.at[at], xb.at[buf, at], x_recv.at[buf, h]).wait()
            for kind, src, dst, to, cond, source in moves:
                if source == buf:

                    @pl.when(cond)
                    def _():
                        x_copy(src, dst, h, kind, to).start()

    ends = []
    total = jnp.int32(0)
    for j in range(lengths.shape[0]):
        total = total + lengths[j]
        ends.append(total)

    def seg(pos):
        out = jnp.zeros(pos.shape, jnp.int32)
        for e in ends:
            out = out + (pos >= e).astype(jnp.int32)
        return out

    q_pos = s * rows + lax.broadcasted_iota(jnp.int32, (rows, 1), 0)
    q_seg = seg(q_pos)

    def project(normed, block):
        return silu_of_twice(dot(normed, w_in[block]) * 0.5).astype(bf16)

    def swap_copy(t):
        return remote(kv.at[t], kv.at[SIB + t], kv_send.at[t], kv_recv.at[t], sibling)

    def shard_of(t, kk):
        ahead = pick(t, {1: ROW * z + kk, 2: ROW * (z - 1) + 2 * p + kk, 3: ROW * (z - 1) + 2 - 2 * p + kk})
        return ahead + pick(t, {0: ROW * z + 2 * p + kk, 4: ROW * (z - 2) + 2 + kk, 5: ROW * (z - 2) + 1 + 2 * p})

    def attend(a):
        side = a // SIB
        t = a % SIB
        shard = shard_of(t, k + side - 2 * k * side)
        k_pos = shard * rows + lax.broadcasted_iota(jnp.int32, (1, rows), 1)
        ok = (k_pos <= q_pos) & (q_pos - k_pos < (WIN - 1) * rows) & (seg(k_pos) == q_seg)
        for h in range(HEADS):
            cols = slice(h * head_dim, (h + 1) * head_dim)
            half = dot_t(q_s[:, cols], kv[a, 0, :, cols]) * half_scale
            weight = jnp.where(ok, silu_of_twice(half), 0.0).astype(bf16)
            acc[:, cols] += dot(weight, kv[a, 1, :, cols])

    w_copies[3].wait()
    kv[0, 0] = project(normed, 3)
    w_copies[1].wait()
    kv[0, 1] = project(normed, 1)

    @pl.when((k == 0) | (p == 1))
    def _():
        swap_copy(0).start()

    def c_round(d):
        low = jnp.maximum(z - d, 0)
        high = jnp.minimum(z + d, depth - 1)
        if isinstance(d, int) and d == 0:
            pl.when(has_above)(lambda: c_block(z, up_send.at[d], above).start())
            pl.when(has_below)(lambda: c_block(z, down_send.at[d], below).start())
            return

        @pl.when(z - d >= 0)
        def _():
            c_block(low, up_send.at[d], above).wait_recv()
            pl.when(has_above)(lambda: c_block(low, up_send.at[d], above).start())

        @pl.when(z + d < depth)
        def _():
            c_block(high, down_send.at[d], below).wait_recv()
            pl.when(has_below)(lambda: c_block(high, down_send.at[d], below).start())

    def c_first():
        c_cross().wait_recv()
        c_round(0)

    w_copies[2].wait()
    q_s[...] = project(normed, 2)
    w_copies[0].wait()
    u_s[...] = project(jnp.concatenate([normed, c_normed], axis=0), 0)
    acc[...] = jnp.zeros_like(acc)
    pl.when(p == 1)(c_first)
    send(0, EARLY, EARLY + 1, p == 1)

    group = part.shape[1]
    lines = group // (2 * cr)

    def c_last():
        def rest(d, carry):
            c_round(d)
            return carry

        lax.fori_loop(3, depth, rest, 0)

    def c_scores():
        pl.when(k == 0)(lambda: swap_copy(0).wait_recv())

        def one(b, carry):
            at = pl.ds(pl.multiple_of(b * lines, lines), lines)
            qc_s[...] = project(cbuf[at, :, :width].reshape(group, width), 2)
            owner = cbuf[at, :, width:].reshape(group, 128)[:, :1].astype(f32)
            part[b] = jnp.zeros((group, width), f32)

            def shard(i, carry):
                t = i // 2
                side = i % 2
                a = t + side * SIB
                near = shard_of(t, k + side - 2 * k * side)
                ok = owner == seg(near * rows + lax.broadcasted_iota(jnp.int32, (1, rows), 1)).astype(f32)
                for h in range(HEADS):
                    cols = slice(h * head_dim, (h + 1) * head_dim)
                    half = dot_t(qc_s[:, cols], kv[a, 0, :, cols]) * half_scale
                    weight = jnp.where(ok, silu_of_twice(half), 0.0).astype(bf16)
                    part[b, :, cols] += dot(weight, kv[a, 1, :, cols])
                return carry

            lax.fori_loop(0, 4, shard, 0)
            out3[at] = part[b].astype(bf16).reshape(lines, 2 * cr, width)
            return carry

        lax.fori_loop(0, depth // lines, one, 0)

        def send(d, c):
            for side in range(2):
                red(d, side).start()
            return c

        lax.fori_loop(1, depth, send, 0)
        red(0, 0).start()

    def red(d, side):
        src = out3.at[(z + d) % depth, pl.ds(side * cr, cr)]
        return remote(src, buf3.at[d], rz_send.at[side, d], rz_recv.at[d], (ROW * (z + d) + 2 * side + k) % n)

    def red_wait(d):
        return remote(out3.at[0, pl.ds(0, cr)], buf3.at[d], rz_send.at[0, d], rz_recv.at[d], partner).wait_recv()

    def only(side, f, *a):
        pl.when(p == side)(functools.partial(f, *a))

    def event(e):
        if e == 1:
            hop(B2, 0)
        if e == 2:
            for h in range(1, PIECES):
                hop(B2, h)
            for h in range(PIECES):
                hop(B1, h)
            if depth > 1:
                only(1, c_round, 1)
            send(3, 0, PIECES // 2)
            only(0, send, 3, PIECES // 2, PIECES)
            only(0, hop, B3, 0)
            only(0, hop, B3, 1)
        if e == 3:
            if depth > 2:
                only(1, c_round, 2)
            only(1, send, 3, PIECES // 2, PIECES)
            only(0, hop, B3, 2)
            only(0, hop, B3, 3)
        if e == 4:
            only(1, c_last)
            only(1, hop, B5, 0)
            only(1, hop, B5, 1)
        if e == 5:
            only(1, hop, B5, 2)
            only(1, hop, B5, 3)
            only(1, c_scores)
        if e == 6:
            for h in range(PIECES):
                only(0, hop, B4, h)
        if e == 7:
            for h in range(PIECES):
                only(1, hop, B3, h)
                only(0, hop, B5, h)

    proj_at = {2: (2, 1), 3: (3, 2), 6: (4, 5), 7: (5, 3)}
    att_at = {
        0: (1, 1),
        1: (1 + SIB, 1 + SIB),
        2: (1 + 2, 1 + 1),
        3: (1 + SIB + 2, 1 + SIB + 1),
        4: (1 + 3, 1 + 2),
        5: (1 + SIB + 3, 1 + SIB + 2),
        6: (0, 1 + 5),
        7: (1 + 5, 1 + 3),
        8: (1 + 4, 1 + SIB + 3),
        9: (1 + SIB + 4, 0),
    }

    def mix(table):
        return {at: v0 * (1 - p) + v1 * p for at, (v0, v1) in table.items()}

    proj_table, att_table = mix(proj_at), mix(att_at)

    def one(e, carry):
        for at in range(10):

            @pl.when(e == at)
            def _():
                event(at)

        t = pick(e, proj_table)

        @pl.when((t > 0) & (z >= t // 2) & ((t < 5) | (k == 0)))
        def _():
            x = xb[t - jnp.minimum(t, 1)]
            kv[t, 0] = project(x, 3)
            kv[t, 1] = project(x, 1)
            pl.when(t < 5)(lambda: swap_copy(t).start())

        a = pick(e, att_table) - 1
        ta = (a + SIB) % SIB
        side = (a + SIB) // SIB - 1

        @pl.when((a >= 0) & (z >= ta // 2) & ((ta < 5) | (k == 0)) & ((ta > 0) | (side < 1) | (k == 1)))
        def _():
            pl.when(side == 1)(lambda: swap_copy(ta).wait_recv())
            attend(a)

        return carry

    lax.fori_loop(0, 10, one, 0)

    w_copies[4].wait()

    def take(d, c):
        red_wait(d)
        return c + buf3[d].astype(f32)

    @pl.when(p == 0)
    def _():
        red_wait(0)

    @pl.when(p == 1)
    def _():
        buf3[0] = out3[z, pl.ds(cr, cr)]

    cattn = lax.fori_loop(1, depth, take, buf3[0].astype(f32))
    y_c = (layer_norm(cattn) * u_s[pl.ds(rows, cr)].astype(f32)).astype(bf16)
    y = (layer_norm(acc[...]) * u_s[pl.ds(0, rows)].astype(f32)).astype(bf16)
    both = dot(jnp.concatenate([y, y_c], axis=0), w_out[...])
    out_ref[pl.ds(0, rows)] = (hist[...].astype(f32) + both[:rows]).astype(bf16)
    out_ref[pl.ds(rows, cr)] = (cand[...].astype(f32) + both[rows:]).astype(bf16)

    for h in range(PIECES):
        for kind, src, dst, to, cond, _ in moves:

            @pl.when(cond)
            def _():
                x_copy(src, dst, h, kind, to).wait_send()

    for t, cond in ((0, (k == 0) | (p == 1)), (1, p == 1), (2, z >= 1), (3, z >= 1), (4, (z >= 2) & (p == 0))):

        @pl.when(cond)
        def _():
            swap_copy(t).wait_send()

    pl.when(p == 0)(lambda: c_cross().wait_send())

    @pl.when(p == 1)
    def _():
        red(0, 0).wait_send()

        def left(d, c):
            pl.when(has_above & (z - d >= 0))(lambda: c_block(0, up_send.at[d], above).wait_send())
            pl.when(has_below & (z + d < depth))(lambda: c_block(0, down_send.at[d], below).wait_send())
            return c

        lax.fori_loop(0, depth, left, 0)

        def sums(d, c):
            for side in range(2):
                red(d, side).wait_send()
            return c

        lax.fori_loop(1, depth, sums, 0)


def hand_out(both, out_ref, cout_ref, held, sem):
    rows, cr = out_ref.shape[0], cout_ref.shape[0]
    parts = (pl.ds(0, rows), pl.ds(rows, cr))
    to = (out_ref, cout_ref)
    loads = [pltpu.make_async_copy(both.at[at], held.at[at], sem.at[i]) for i, at in enumerate(parts)]
    saves = [pltpu.make_async_copy(held.at[at], to[i], sem.at[i]) for i, at in enumerate(parts)]
    for c in loads:
        c.start()
    for i in range(2):
        loads[i].wait()
        saves[i].start()
    for c in saves:
        c.wait()


def per_device(n, history, candidates, lengths, cand_user, w_in, w_out):
    rows, width = history.shape
    cr = candidates.shape[0]
    depth = n // ROW
    users = cand_user[None, :]
    vmem = pl.BlockSpec(memory_space=pltpu.VMEM)
    dma = pltpu.SemaphoreType.DMA
    block = depth * 2 * cr
    group = min(block, 256)
    both = pl.pallas_call(
        functools.partial(kernel, n),
        out_shape=jax.ShapeDtypeStruct((rows + cr, width), bf16),
        in_specs=[
            pl.BlockSpec(memory_space=pltpu.SMEM),
            vmem,
            vmem,
            vmem,
            pl.BlockSpec(memory_space=pl.ANY),
            pl.BlockSpec(memory_space=pl.ANY),
        ],
        out_specs=vmem,
        scratch_shapes=[
            pltpu.VMEM((4, width, width), bf16),
            pltpu.VMEM((width, width), bf16),
            pltpu.VMEM((rows, width), bf16),
            pltpu.VMEM((5, rows, width), bf16),
            pltpu.VMEM((SIB + 5, 2, rows, width), bf16),
            pltpu.VMEM((rows, width), bf16),
            pltpu.VMEM((rows + cr, width), bf16),
            pltpu.VMEM((rows, width), f32),
            pltpu.VMEM((cr, width + 128), bf16),
            pltpu.VMEM((depth, 2 * cr, width + 128), bf16),
            pltpu.VMEM((group, width), bf16),
            pltpu.VMEM((block // group, group, width), f32),
            pltpu.VMEM((depth, 2 * cr, width), bf16),
            pltpu.VMEM((depth, cr, width), bf16),
            dma((5,)),
            dma((6, PIECES)),
            dma((5, PIECES)),
            dma((5,)),
            dma((5,)),
            dma((1,)),
            dma((depth + 1,)),
            dma((depth,)),
            dma((depth,)),
            dma((2, depth)),
            dma((depth,)),
        ],
        compiler_params=pltpu.CompilerParams(
            collective_id=0, has_side_effects=True, vmem_limit_bytes=60 * 1024 * 1024
        ),
    )(lengths, history, candidates, users, w_in, w_out)
    hbm = pl.BlockSpec(memory_space=pl.ANY)
    return pl.pallas_call(
        hand_out,
        out_shape=(
            jax.ShapeDtypeStruct((rows, width), bf16),
            jax.ShapeDtypeStruct((cr, width), bf16),
        ),
        in_specs=[hbm],
        out_specs=(hbm, hbm),
        scratch_shapes=[pltpu.VMEM((rows + cr, width), bf16), dma((2,))],
    )(both)


def solution(mesh):
    n = mesh.shape["seq"]
    placed = (
        P(("grp", "seq"), None),
        P(("grp", "seq"), None),
        P("grp"),
        P(("grp", "seq")),
        P(),
        P(),
    )
    return jax.shard_map(
        functools.partial(per_device, n),
        mesh=mesh,
        in_specs=placed,
        out_specs=(P(("grp", "seq"), None), P(("grp", "seq"), None)),
        check_vma=False,
    )
```

```python
import functools

import jax
import jax.numpy as jnp
from jax import lax
from jax.experimental import pallas as pl
from jax.experimental.pallas import tpu as pltpu
from jax.sharding import PartitionSpec as P

HEADS = 8
WIN = 8
PIECES = 4
ROW = 4
EARLY = 3
SIB = 6
B1, B2, B3, B4, B5 = 0, 1, 2, 3, 4

eps = 1e-06
bf16 = jnp.bfloat16
f32 = jnp.float32


def layer_norm(rows):
    centred = rows - jnp.mean(rows, axis=-1, keepdims=True)
    return centred * lax.rsqrt(jnp.mean(centred * centred, axis=-1, keepdims=True) + eps)


def silu_of_twice(half):
    return half + half * jnp.tanh(half)


def dot(a, b):
    return jnp.dot(a, b, preferred_element_type=f32)


def dot_t(a, b):
    return lax.dot_general(a, b, (((1,), (1,)), ((), ())), preferred_element_type=f32)


def pick(i, entries):
    out = 0
    for at, value in entries.items():
        out = out + value * (1 - jnp.minimum((i - at) * (i - at), 1))
    return out


def kernel(
    n,
    lengths_hbm,
    hist_hbm,
    cand_hbm,
    users_hbm,
    w_in_hbm,
    w_out_hbm,
    out_ref,
    lengths,
    hist,
    cand,
    users_row,
    in_sem,
    w_in,
    w_out,
    own,
    xb,
    kv,
    q_s,
    u_s,
    acc,
    cmsg,
    cbuf,
    qc_s,
    part,
    out3,
    buf3,
    w_sem,
    x_send,
    x_recv,
    kv_send,
    kv_recv,
    c_send,
    c_recv,
    up_send,
    down_send,
    rz_send,
    rz_recv,
):
    rows, width = hist.shape
    cr = cand.shape[0]
    head_dim = width // HEADS
    half_scale = 0.5 * head_dim ** (-0.5)
    depth = n // ROW
    s = lax.axis_index("seq")
    z = s // ROW
    r = s % ROW
    p = r // 2
    k = r % 2
    piece = rows // PIECES
    sibling = s + 1 - 2 * k
    partner = s + 2 - 4 * p
    above = (s + ROW) % n
    below = (s + n - ROW) % n
    has_above = z + 1 < depth
    has_below = z >= 1

    in_copies = [
        pltpu.make_async_copy(src, dst, in_sem.at[i])
        for i, (src, dst) in enumerate(
            ((hist_hbm, hist), (cand_hbm, cand), (users_hbm, users_row), (lengths_hbm, lengths))
        )
    ]
    for c in in_copies:
        c.start()
    w_copies = [
        pltpu.make_async_copy(
            w_in_hbm.at[0, :, pl.ds(c * width, width)], w_in.at[c], w_sem.at[c]
        )
        for c in range(4)
    ]
    w_copies.append(pltpu.make_async_copy(w_out_hbm.at[0], w_out, w_sem.at[4]))
    barrier = pltpu.get_barrier_semaphore()

    def greet(to):
        pl.semaphore_signal(barrier, inc=1, device_id={"seq": to}, device_id_type=pl.DeviceIdType.MESH)

    peers = (
        (None, sibling),
        (None, partner),
        (has_above, above),
        (has_below, below),
        (has_above & (r == 1), (s + 3) % n),
        (has_below & (r == 0), (s + n - 3) % n),
    )
    for cond, to in peers:
        if cond is None:
            greet(to)
        else:
            pl.when(cond)(functools.partial(greet, to))

    for c in (3, 1, 2, 0, 4):
        w_copies[c].start()
    for c in in_copies[1:]:
        c.wait()

    eye = lax.broadcasted_iota(jnp.int32, (cr, cr), 0) == lax.broadcasted_iota(jnp.int32, (cr, cr), 1)
    column = jnp.sum(jnp.where(eye, users_row[...], 0), axis=1, keepdims=True)
    c_normed = layer_norm(cand[...].astype(f32)).astype(bf16)
    cmsg[:, :width] = c_normed
    cmsg[:, width:] = jnp.broadcast_to(column, (cr, 128)).astype(f32).astype(bf16)

    @pl.when(p == 1)
    def _():
        cbuf[z, pl.ds(cr, cr)] = cmsg[...]

    in_copies[0].wait()
    normed = layer_norm(hist[...].astype(f32)).astype(bf16)
    own[...] = normed

    @pl.when((p == 1) & (z == 0))
    def _():
        xb[B2] = jnp.zeros((rows, width), bf16)

    @pl.when((p == 1) & (k == 0) & (z == 1))
    def _():
        xb[B5] = jnp.zeros((rows, width), bf16)

    pl.semaphore_wait(barrier, sum(1 if cond is None else cond.astype(jnp.int32) for cond, _ in peers))

    def remote(src, dst, send, recv, to):
        return pltpu.make_async_remote_copy(
            src_ref=src,
            dst_ref=dst,
            send_sem=send,
            recv_sem=recv,
            device_id={"seq": to},
            device_id_type=pl.DeviceIdType.MESH,
        )

    def x_copy(src, dst, h, kind, to):
        at = pl.ds(h * piece, piece)
        return remote(src.at[at], xb.at[dst, at], x_send.at[kind, h], x_recv.at[dst, h], to)

    moves = (
        (0, own, B2, above, has_above, None),
        (1, own, B1, partner, p == 0, None),
        (2, xb.at[B2], B3, partner, has_below, B2),
        (3, xb.at[B2], B5, (s + 3 + p) % n, has_below & has_above & (k == 1), None),
        (4, xb.at[B3], B4, above, has_below & has_above & (r == 0), B3),
        (5, xb.at[B5], B4, partner, (z >= 2) & (r == 3), B5),
        (6, xb.at[B5], B5, sibling, (z >= 2) & (r == 3), B5),
    )
    arrives = {
        B1: p == 1,
        B2: has_below,
        B3: has_below,
        B4: (z >= 2) & (p == 0),
        B5: (z >= 2) & ((k == 0) | (p == 1)),
    }

    def c_cross():
        return remote(cmsg, cbuf.at[z, pl.ds(0, cr)], c_send.at[0], c_recv.at[depth], partner)

    def c_block(block, send, to):
        return remote(cbuf.at[block], cbuf.at[block], send, c_recv.at[block], to)

    @pl.when(p == 0)
    def _():
        c_cross().start()

    def send(which, first, last, also=None):
        kind, src, dst, to, cond, _ = moves[which]

        @pl.when(cond if also is None else cond & also)
        def _():
            for h in range(first, last):
                x_copy(src, dst, h, kind, to).start()

    for h in range(PIECES):
        send(0, h, h + 1, None if h < EARLY else p == 0)
        send(1, h, h + 1)

    def hop(buf, h):
        at = pl.ds(h * piece, piece)

        @pl.when(arrives[buf])
        def _():
            pltpu.make_async_copy(hist.at[at], xb.at[buf, at], x_recv.at[buf, h]).wait()
            for kind, src, dst, to, cond, source in moves:
                if source == buf:

                    @pl.when(cond)
                    def _():
                        x_copy(src, dst, h, kind, to).start()

    ends = []
    total = jnp.int32(0)
    for j in range(lengths.shape[0]):
        total = total + lengths[j]
        ends.append(total)

    def seg(pos):
        out = jnp.zeros(pos.shape, jnp.int32)
        for e in ends:
            out = out + (pos >= e).astype(jnp.int32)
        return out

    q_pos = s * rows + lax.broadcasted_iota(jnp.int32, (rows, 1), 0)
    q_seg = seg(q_pos)

    def project(normed, block):
        return silu_of_twice(dot(normed, w_in[block]) * 0.5).astype(bf16)

    half = rows // 2
    low = pl.ds(0, half)
    high = pl.ds(half, half)

    def swap_copy(t):
        return remote(kv.at[t], kv.at[SIB + t], kv_send.at[t], kv_recv.at[t], sibling)

    def swap_half(t):
        to = low if t == 3 else high
        return remote(kv.at[t, :, low], kv.at[SIB + 3, :, to], kv_send.at[t], kv_recv.at[t], sibling)

    def bases(t, side):
        kk = k + side - 2 * k * side
        first = ROW * (z - 1 + p) + kk
        second = ROW * (z - 1) + 2 + kk
        late = ROW * (z - 2 + p) + 2 - 2 * p + kk
        lone = ROW * (z - 2) + 1 + 2 * p
        mine = s + side * (1 - 2 * k)
        whole = k * (1 - side) + side
        h = half
        a = pick(t, {0: mine * rows, 1: first * rows, 2: first * rows + h, 3: late * rows, 4: late * rows + h})
        b = pick(
            t,
            {
                0: mine * rows + h,
                1: second * rows,
                2: second * rows + h,
                3: (1 - whole) * lone * rows + whole * (late * rows + h),
                4: lone * rows + h,
            },
        )
        return a, b

    def attend(a):
        start, later = bases(a % SIB, a // SIB)
        lane = lax.broadcasted_iota(jnp.int32, (1, rows), 1)
        k_pos = jnp.where(lane < half, start + lane, later + lane - half)
        ok = (k_pos <= q_pos) & (q_pos - k_pos < (WIN - 1) * rows) & (seg(k_pos) == q_seg)
        for h in range(HEADS):
            cols = slice(h * head_dim, (h + 1) * head_dim)
            score = dot_t(q_s[:, cols], kv[a, 0, :, cols]) * half_scale
            weight = jnp.where(ok, silu_of_twice(score), 0.0).astype(bf16)
            acc[:, cols] += dot(weight, kv[a, 1, :, cols])

    w_copies[3].wait()
    kv[0, 0] = project(normed, 3)
    w_copies[1].wait()
    kv[0, 1] = project(normed, 1)

    @pl.when((k == 0) | (p == 1))
    def _():
        swap_copy(0).start()

    def c_round(d):
        low = jnp.maximum(z - d, 0)
        high = jnp.minimum(z + d, depth - 1)
        if isinstance(d, int) and d == 0:
            pl.when(has_above)(lambda: c_block(z, up_send.at[d], above).start())
            pl.when(has_below)(lambda: c_block(z, down_send.at[d], below).start())
            return

        @pl.when(z - d >= 0)
        def _():
            c_block(low, up_send.at[d], above).wait_recv()
            pl.when(has_above)(lambda: c_block(low, up_send.at[d], above).start())

        @pl.when(z + d < depth)
        def _():
            c_block(high, down_send.at[d], below).wait_recv()
            pl.when(has_below)(lambda: c_block(high, down_send.at[d], below).start())

    def c_first():
        c_cross().wait_recv()
        c_round(0)

    w_copies[2].wait()
    q_s[...] = project(normed, 2)
    w_copies[0].wait()
    u_s[...] = project(jnp.concatenate([normed, c_normed], axis=0), 0)
    acc[...] = jnp.zeros_like(acc)
    pl.when(p == 1)(c_first)
    send(0, EARLY, EARLY + 1, p == 1)

    group = part.shape[1]
    lines = group // (2 * cr)

    def c_last():
        def rest(d, carry):
            c_round(d)
            return carry

        lax.fori_loop(3, depth, rest, 0)

    def c_scores():
        pl.when(k == 0)(lambda: swap_copy(0).wait_recv())

        def one(g, carry):
            at = pl.ds(pl.multiple_of(g * lines, lines), lines)
            qc_s[...] = project(cbuf[at, :, :width].reshape(group, width), 2)
            owner = cbuf[at, :, width:].reshape(group, 128)[:, :1].astype(f32)
            part[g] = jnp.zeros((group, width), f32)

            def shard(i, carry):
                for at in (2, 3):
                    pl.when((r == 3) & (g == 0) & (i == 2 * at - 3))(functools.partial(hop, B5, at))
                t = i // 2
                side = i % 2
                a = t + side * SIB
                b = 2 * t + side * SIB
                rest = pl.ds(pl.multiple_of((1 - t) * half, half), half)
                near = ROW * z + 2 - 2 * t + k + side - 2 * k * side
                ok = owner == seg(near * rows + lax.broadcasted_iota(jnp.int32, (1, rows), 1)).astype(f32)
                for h in range(HEADS):
                    cols = slice(h * head_dim, (h + 1) * head_dim)
                    keys = jnp.concatenate([kv[a, 0, low, cols], kv[b, 0, rest, cols]], axis=0)
                    values = jnp.concatenate([kv[a, 1, low, cols], kv[b, 1, rest, cols]], axis=0)
                    score = dot_t(qc_s[...][:, cols], keys) * half_scale
                    weight = jnp.where(ok, silu_of_twice(score), 0.0).astype(bf16)
                    part[g, :, cols] += dot(weight, values)
                return carry

            lax.fori_loop(0, 4, shard, 0)
            out3[at] = part[g].astype(bf16).reshape(lines, 2 * cr, width)
            return carry

        lax.fori_loop(0, depth // lines, one, 0)

        def send(d, c):
            for side in range(2):
                red(d, side).start()
            return c

        lax.fori_loop(1, depth, send, 0)
        red(0, 0).start()

    def red(d, side):
        src = out3.at[(z + d) % depth, pl.ds(side * cr, cr)]
        return remote(src, buf3.at[d], rz_send.at[side, d], rz_recv.at[d], (ROW * (z + d) + 2 * side + k) % n)

    def red_wait(d):
        return remote(out3.at[0, pl.ds(0, cr)], buf3.at[d], rz_send.at[0, d], rz_recv.at[d], partner).wait_recv()

    def only(side, f, *a):
        pl.when(p == side if side < 2 else r == side)(functools.partial(f, *a))

    def event(e):
        if e == 1:
            hop(B2, 0)
        if e == 2:
            hop(B2, 1)
            only(0, hop, B2, 2)
            for h in (0, 1):
                hop(B1, h)
                only(0, hop, B3, h)
        if e == 3:
            only(1, hop, B2, 2)
            only(0, hop, B2, 3)
            only(0, send, 3, 0, PIECES)
        if e == 4:
            only(1, hop, B2, 3)
            for h in (2, 3):
                hop(B1, h)
                only(0, hop, B3, h)
            if depth > 1:
                only(1, c_round, 1)
            only(1, send, 3, 0, PIECES // 2)
        if e == 5:
            if depth > 2:
                only(3, c_round, 2)
            only(1, send, 3, PIECES // 2, PIECES)
            only(3, hop, B5, 0)
            only(3, hop, B5, 1)
        if e == 6:
            only(3, c_last)
            only(3, c_scores)
            if depth > 2:
                only(2, c_round, 2)
            for h in (0, 1):
                only(2, hop, B5, h)
                only(1, hop, B3, h)
                only(0, hop, B4, h)
                only(0, hop, B5, h)
            late(1)
        if e == 7:
            only(2, c_last)
            only(2, c_scores)
            late(0)

    def late(core):
        @pl.when(k == core)
        def _():
            for h in (2, 3):
                only(2, hop, B5, h)
                only(1, hop, B3, h)
                only(0, hop, B4, h)
                only(0, hop, B5, h)

    proj_table = {2: 1, 4: 2, 6: 3, 7: 4}
    att_table = {
        0: 1,
        1: 1 + SIB,
        2: 1 + 1,
        3: 1 + SIB + 1,
        4: 1 + 2,
        5: 1 + SIB + 2,
        6: 1 + 3,
        7: 1 + 4,
        8: 1 + SIB + 3,
    }

    def live(t):
        return z >= jnp.minimum(t, 1) * (1 - p) + t // 3

    def one(e, carry):
        for at in range(9):

            @pl.when(e == at)
            def _():
                event(at)

        t = pick(e, proj_table)

        @pl.when((t > 0) & live(t) & ((t < 4) | (k == 0)))
        def _():
            end = t // 3
            one_at = (1 - end) * (1 - p) + end * (3 - p)
            two_at = (1 - end) * (2 - p) + end * (4 * (1 - k) + (3 - p) * k)
            one_off = (t + 1) % 2
            two_off = jnp.maximum(one_off, end * k)
            x1 = xb[one_at, pl.ds(pl.multiple_of(one_off * half, half), half)]
            x2 = xb[two_at, pl.ds(pl.multiple_of(two_off * half, half), half)]
            x = jnp.concatenate([x1, x2], axis=0)
            kv[t, 0] = project(x, 3)
            kv[t, 1] = project(x, 1)
            pl.when((t < 3) | ((t == 3) & (k == 1)))(lambda: swap_copy(t).start())
            pl.when((t == 3) & (k == 0))(lambda: swap_half(3).start())
            pl.when((t == 4) & (k == 0))(lambda: swap_half(4).start())

        a = pick(e, att_table) - 1
        ta = a % SIB
        side = a // SIB

        @pl.when(live(ta) & ((ta < 4) | (k == 0)) & ((ta > 0) | (side < 1) | (k == 1)))
        def _():
            pl.when((side == 1) & ((ta < 3) | (k == 0)))(lambda: swap_copy(ta).wait_recv())

            @pl.when((side == 1) & (ta == 3) & (k == 1))
            def _():
                swap_half(3).wait_recv()
                swap_half(4).wait_recv()

            attend(a)

        return carry

    lax.fori_loop(0, 9, one, 0)

    w_copies[4].wait()

    def take(d, c):
        red_wait(d)
        return c + buf3[d].astype(f32)

    @pl.when(p == 0)
    def _():
        red_wait(0)

    @pl.when(p == 1)
    def _():
        buf3[0] = out3[z, pl.ds(cr, cr)]

    cattn = lax.fori_loop(1, depth, take, buf3[0].astype(f32))
    y_c = (layer_norm(cattn) * u_s[pl.ds(rows, cr)].astype(f32)).astype(bf16)
    y = (layer_norm(acc[...]) * u_s[pl.ds(0, rows)].astype(f32)).astype(bf16)
    both = dot(jnp.concatenate([y, y_c], axis=0), w_out[...])
    out_ref[pl.ds(0, rows)] = (hist[...].astype(f32) + both[:rows]).astype(bf16)
    out_ref[pl.ds(rows, cr)] = (cand[...].astype(f32) + both[rows:]).astype(bf16)

    for h in range(PIECES):
        for kind, src, dst, to, cond, _ in moves:

            @pl.when(cond)
            def _():
                x_copy(src, dst, h, kind, to).wait_send()

    for t, cond in ((0, (k == 0) | (p == 1)), (1, live(1)), (2, live(2)), (3, live(3) & (k == 1))):

        @pl.when(cond)
        def _():
            swap_copy(t).wait_send()

    @pl.when(live(3) & (k == 0))
    def _():
        swap_half(3).wait_send()
        swap_half(4).wait_send()

    pl.when(p == 0)(lambda: c_cross().wait_send())

    @pl.when(p == 1)
    def _():
        red(0, 0).wait_send()

        def left(d, c):
            pl.when(has_above & (z - d >= 0))(lambda: c_block(0, up_send.at[d], above).wait_send())
            pl.when(has_below & (z + d < depth))(lambda: c_block(0, down_send.at[d], below).wait_send())
            return c

        lax.fori_loop(0, depth, left, 0)

        def sums(d, c):
            for side in range(2):
                red(d, side).wait_send()
            return c

        lax.fori_loop(1, depth, sums, 0)


def hand_out(both, out_ref, cout_ref, sem):
    rows, cr = out_ref.shape[0], cout_ref.shape[0]
    parts = (pl.ds(0, rows), pl.ds(rows, cr))
    to = (out_ref, cout_ref)
    saves = [pltpu.make_async_copy(both.at[at], to[i], sem.at[i]) for i, at in enumerate(parts)]
    for c in saves:
        c.start()
    for c in saves:
        c.wait()


def per_device(n, history, candidates, lengths, cand_user, w_in, w_out):
    rows, width = history.shape
    cr = candidates.shape[0]
    depth = n // ROW
    users = cand_user[None, :]
    vmem = pl.BlockSpec(memory_space=pltpu.VMEM)
    dma = pltpu.SemaphoreType.DMA
    block = depth * 2 * cr
    group = min(block, 256)
    both = pl.pallas_call(
        functools.partial(kernel, n),
        out_shape=jax.ShapeDtypeStruct((rows + cr, width), bf16),
        in_specs=[pl.BlockSpec(memory_space=pltpu.HBM)] * 6,
        out_specs=vmem,
        scratch_shapes=[
            pltpu.SMEM(lengths.shape, jnp.int32),
            pltpu.VMEM((rows, width), bf16),
            pltpu.VMEM((cr, width), bf16),
            pltpu.VMEM((1, cr), jnp.int32),
            dma((4,)),
            pltpu.VMEM((4, width, width), bf16),
            pltpu.VMEM((width, width), bf16),
            pltpu.VMEM((rows, width), bf16),
            pltpu.VMEM((5, rows, width), bf16),
            pltpu.VMEM((SIB + 5, 2, rows, width), bf16),
            pltpu.VMEM((rows, width), bf16),
            pltpu.VMEM((rows + cr, width), bf16),
            pltpu.VMEM((rows, width), f32),
            pltpu.VMEM((cr, width + 128), bf16),
            pltpu.VMEM((depth, 2 * cr, width + 128), bf16),
            pltpu.VMEM((group, width), bf16),
            pltpu.VMEM((block // group, group, width), f32),
            pltpu.VMEM((depth, 2 * cr, width), bf16),
            pltpu.VMEM((depth, cr, width), bf16),
            dma((5,)),
            dma((7, PIECES)),
            dma((5, PIECES)),
            dma((5,)),
            dma((5,)),
            dma((1,)),
            dma((depth + 1,)),
            dma((depth,)),
            dma((depth,)),
            dma((2, depth)),
            dma((depth,)),
        ],
        compiler_params=pltpu.CompilerParams(
            collective_id=0, has_side_effects=True, vmem_limit_bytes=52 * 1024 * 1024
        ),
    )(*(pltpu.with_memory_space_constraint(x, pltpu.HBM) for x in (lengths, history, candidates, users, w_in, w_out)))
    hbm = pl.BlockSpec(memory_space=pl.ANY)
    return pl.pallas_call(
        hand_out,
        out_shape=(
            jax.ShapeDtypeStruct((rows, width), bf16),
            jax.ShapeDtypeStruct((cr, width), bf16),
        ),
        in_specs=[vmem],
        out_specs=(hbm, hbm),
        scratch_shapes=[dma((2,))],
        compiler_params=pltpu.CompilerParams(vmem_limit_bytes=2 * 1024 * 1024),
    )(both)


def solution(mesh):
    n = mesh.shape["seq"]
    placed = (
        P(("grp", "seq"), None),
        P(("grp", "seq"), None),
        P("grp"),
        P(("grp", "seq")),
        P(),
        P(),
    )
    return jax.shard_map(
        functools.partial(per_device, n),
        mesh=mesh,
        in_specs=placed,
        out_specs=(P(("grp", "seq"), None), P(("grp", "seq"), None)),
        check_vma=False,
    )
```

```python
import functools

import jax
import jax.numpy as jnp
from jax import lax
from jax.experimental import pallas as pl
from jax.experimental.pallas import tpu as pltpu
from jax.sharding import PartitionSpec as P

HEADS = 8
WIN = 8
PIECES = 4
ROW = 4
EARLY = 3
SIB = 6
B1, B2, B3, B4, B5 = 0, 1, 2, 3, 4

eps = 1e-06
bf16 = jnp.bfloat16
f32 = jnp.float32


def layer_norm(rows):
    centred = rows - jnp.mean(rows, axis=-1, keepdims=True)
    return centred * lax.rsqrt(jnp.mean(centred * centred, axis=-1, keepdims=True) + eps)


def silu_of_twice(half):
    return half + half * jnp.tanh(half)


def dot(a, b):
    return jnp.dot(a, b, preferred_element_type=f32)


def dot_t(a, b):
    return lax.dot_general(a, b, (((1,), (1,)), ((), ())), preferred_element_type=f32)


def pick(i, entries):
    out = 0
    for at, value in entries.items():
        out = out + value * (1 - jnp.minimum((i - at) * (i - at), 1))
    return out


def kernel(
    n,
    lengths_hbm,
    hist_hbm,
    cand_hbm,
    users_hbm,
    w_in_hbm,
    w_out_hbm,
    out_ref,
    lengths,
    hist,
    cand,
    users_row,
    in_sem,
    w_in,
    w_out,
    own,
    xb,
    kv,
    q_s,
    u_s,
    acc,
    cmsg,
    cbuf,
    qc_s,
    part,
    out3,
    buf3,
    w_sem,
    x_send,
    x_recv,
    kv_send,
    kv_recv,
    c_send,
    c_recv,
    up_send,
    down_send,
    rz_send,
    rz_recv,
):
    rows, width = hist.shape
    cr = cand.shape[0]
    head_dim = width // HEADS
    half_scale = 0.5 * head_dim ** (-0.5)
    depth = n // ROW
    s = lax.axis_index("seq")
    z = s // ROW
    r = s % ROW
    p = r // 2
    k = r % 2
    piece = rows // PIECES
    sibling = s + 1 - 2 * k
    partner = s + 2 - 4 * p
    above = (s + ROW) % n
    below = (s + n - ROW) % n
    has_above = z + 1 < depth
    has_below = z >= 1

    in_copies = [
        pltpu.make_async_copy(src, dst, in_sem.at[i])
        for i, (src, dst) in enumerate(
            ((hist_hbm, hist), (cand_hbm, cand), (users_hbm, users_row), (lengths_hbm, lengths))
        )
    ]
    for c in in_copies:
        c.start()
    w_copies = [
        pltpu.make_async_copy(
            w_in_hbm.at[0, :, pl.ds(c * width, width)], w_in.at[c], w_sem.at[c]
        )
        for c in range(4)
    ]
    w_copies.append(pltpu.make_async_copy(w_out_hbm.at[0], w_out, w_sem.at[4]))
    barrier = pltpu.get_barrier_semaphore()

    def greet(to):
        pl.semaphore_signal(barrier, inc=1, device_id={"seq": to}, device_id_type=pl.DeviceIdType.MESH)

    peers = (
        (None, sibling),
        (None, partner),
        (has_above, above),
        (has_below, below),
        (has_above & (r == 1), (s + 3) % n),
        (has_below & (r == 0), (s + n - 3) % n),
    )
    for cond, to in peers:
        if cond is None:
            greet(to)
        else:
            pl.when(cond)(functools.partial(greet, to))

    for c in (3, 1, 2, 0, 4):
        w_copies[c].start()
    for c in in_copies[1:]:
        c.wait()

    eye = lax.broadcasted_iota(jnp.int32, (cr, cr), 0) == lax.broadcasted_iota(jnp.int32, (cr, cr), 1)
    column = jnp.sum(jnp.where(eye, users_row[...], 0), axis=1, keepdims=True)
    c_normed = layer_norm(cand[...].astype(f32)).astype(bf16)
    cmsg[:, :width] = c_normed
    cmsg[:, width:] = jnp.broadcast_to(column, (cr, 128)).astype(f32).astype(bf16)

    @pl.when(p == 1)
    def _():
        cbuf[z, pl.ds(cr, cr)] = cmsg[...]

    in_copies[0].wait()
    normed = layer_norm(hist[...].astype(f32)).astype(bf16)
    own[...] = normed

    @pl.when((p == 1) & (z == 0))
    def _():
        xb[B2] = jnp.zeros((rows, width), bf16)

    @pl.when((p == 1) & (k == 0) & (z == 1))
    def _():
        xb[B5] = jnp.zeros((rows, width), bf16)

    pl.semaphore_wait(barrier, sum(1 if cond is None else cond.astype(jnp.int32) for cond, _ in peers))

    def remote(src, dst, send, recv, to):
        return pltpu.make_async_remote_copy(
            src_ref=src,
            dst_ref=dst,
            send_sem=send,
            recv_sem=recv,
            device_id={"seq": to},
            device_id_type=pl.DeviceIdType.MESH,
        )

    def x_copy(src, dst, h, kind, to):
        at = pl.ds(h * piece, piece)
        return remote(src.at[at], xb.at[dst, at], x_send.at[kind, h], x_recv.at[dst, h], to)

    moves = (
        (0, own, B2, above, has_above, None),
        (1, own, B1, partner, p == 0, None),
        (2, xb.at[B2], B3, partner, has_below, B2),
        (3, xb.at[B2], B5, (s + 3 + p) % n, has_below & has_above & (k == 1), None),
        (4, xb.at[B3], B4, above, has_below & has_above & (r == 0), B3),
        (5, xb.at[B5], B4, partner, (z >= 2) & (r == 3), B5),
        (7, xb.at[B3], B4, above, has_below & has_above & (r == 1), B3),
        (6, xb.at[B5], B5, sibling, (z >= 2) & (r == 3), B5),
    )
    arrives = {
        B1: p == 1,
        B2: has_below,
        B3: has_below,
        B4: (z >= 2) & (p == 0),
        B5: (z >= 2) & ((k == 0) | (p == 1)),
    }

    def c_cross():
        return remote(cmsg, cbuf.at[z, pl.ds(0, cr)], c_send.at[0], c_recv.at[depth], partner)

    def c_block(block, send, to):
        return remote(cbuf.at[block], cbuf.at[block], send, c_recv.at[block], to)

    @pl.when(p == 0)
    def _():
        c_cross().start()

    def send(which, first, last, also=None):
        kind, src, dst, to, cond, _ = moves[which]

        @pl.when(cond if also is None else cond & also)
        def _():
            for h in range(first, last):
                x_copy(src, dst, h, kind, to).start()

    for h in range(PIECES):
        send(0, h, h + 1, None if h < EARLY else p == 0)
        send(1, h, h + 1)

    def routed(kind, h):
        return {5: h < PIECES - 1, 7: h == PIECES - 1}.get(kind, True)

    def hop(buf, h):
        at = pl.ds(h * piece, piece)

        @pl.when(arrives[buf])
        def _():
            pltpu.make_async_copy(hist.at[at], xb.at[buf, at], x_recv.at[buf, h]).wait()
            for kind, src, dst, to, cond, source in moves:
                if source == buf and routed(kind, h):

                    @pl.when(cond)
                    def _():
                        x_copy(src, dst, h, kind, to).start()

    ends = []
    total = jnp.int32(0)
    for j in range(lengths.shape[0]):
        total = total + lengths[j]
        ends.append(total)

    def seg(pos):
        out = jnp.zeros(pos.shape, jnp.int32)
        for e in ends:
            out = out + (pos >= e).astype(jnp.int32)
        return out

    q_pos = s * rows + lax.broadcasted_iota(jnp.int32, (rows, 1), 0)
    q_seg = seg(q_pos)

    def project(normed, block):
        return silu_of_twice(dot(normed, w_in[block]) * 0.5).astype(bf16)

    half = rows // 2
    low = pl.ds(0, half)
    high = pl.ds(half, half)

    def swap_copy(t):
        return remote(kv.at[t], kv.at[SIB + t], kv_send.at[t], kv_recv.at[t], sibling)

    def swap_half(t):
        to = low if t == 3 else high
        return remote(kv.at[t, :, low], kv.at[SIB + 3, :, to], kv_send.at[t], kv_recv.at[t], sibling)

    def bases(t, side):
        kk = k + side - 2 * k * side
        first = ROW * (z - 1 + p) + kk
        second = ROW * (z - 1) + 2 + kk
        late = ROW * (z - 2 + p) + 2 - 2 * p + kk
        lone = ROW * (z - 2) + 1 + 2 * p
        mine = s + side * (1 - 2 * k)
        whole = k * (1 - side) + side
        h = half
        a = pick(t, {0: mine * rows, 1: first * rows, 2: first * rows + h, 3: late * rows, 4: late * rows + h})
        b = pick(
            t,
            {
                0: mine * rows + h,
                1: second * rows,
                2: second * rows + h,
                3: (1 - whole) * lone * rows + whole * (late * rows + h),
                4: lone * rows + h,
            },
        )
        return a, b

    def attend(a):
        start, later = bases(a % SIB, a // SIB)
        lane = lax.broadcasted_iota(jnp.int32, (1, rows), 1)
        k_pos = jnp.where(lane < half, start + lane, later + lane - half)
        ok = (k_pos <= q_pos) & (q_pos - k_pos < (WIN - 1) * rows) & (seg(k_pos) == q_seg)
        for h in range(HEADS):
            cols = slice(h * head_dim, (h + 1) * head_dim)
            score = dot_t(q_s[:, cols], kv[a, 0, :, cols]) * half_scale
            weight = jnp.where(ok, silu_of_twice(score), 0.0).astype(bf16)
            acc[:, cols] += dot(weight, kv[a, 1, :, cols])

    w_copies[3].wait()
    kv[0, 0] = project(normed, 3)
    w_copies[1].wait()
    kv[0, 1] = project(normed, 1)

    @pl.when((k == 0) | (p == 1))
    def _():
        swap_copy(0).start()

    def c_round(d):
        low = jnp.maximum(z - d, 0)
        high = jnp.minimum(z + d, depth - 1)
        if isinstance(d, int) and d == 0:
            pl.when(has_above)(lambda: c_block(z, up_send.at[d], above).start())
            pl.when(has_below)(lambda: c_block(z, down_send.at[d], below).start())
            return

        @pl.when(z - d >= 0)
        def _():
            c_block(low, up_send.at[d], above).wait_recv()
            pl.when(has_above)(lambda: c_block(low, up_send.at[d], above).start())

        @pl.when(z + d < depth)
        def _():
            c_block(high, down_send.at[d], below).wait_recv()
            pl.when(has_below)(lambda: c_block(high, down_send.at[d], below).start())

    def c_first():
        c_cross().wait_recv()
        c_round(0)

    w_copies[2].wait()
    q_s[...] = project(normed, 2)
    w_copies[0].wait()
    u_s[...] = project(jnp.concatenate([normed, c_normed], axis=0), 0)
    acc[...] = jnp.zeros_like(acc)
    pl.when(p == 1)(c_first)
    send(0, EARLY, EARLY + 1, p == 1)

    group = part.shape[1]
    lines = group // (2 * cr)

    def c_last():
        def rest(d, carry):
            c_round(d)
            return carry

        lax.fori_loop(3, depth, rest, 0)

    def c_scores():
        pl.when(k == 0)(lambda: swap_copy(0).wait_recv())

        def one(g, carry):
            at = pl.ds(pl.multiple_of(g * lines, lines), lines)
            qc_s[...] = project(cbuf[at, :, :width].reshape(group, width), 2)
            owner = cbuf[at, :, width:].reshape(group, 128)[:, :1].astype(f32)
            part[g] = jnp.zeros((group, width), f32)

            def shard(i, carry):
                for at in (2, 3):
                    pl.when((r == 3) & (g == 0) & (i == 2 * at - 3))(functools.partial(hop, B5, at))
                t = i // 2
                side = i % 2
                a = t + side * SIB
                b = 2 * t + side * SIB
                rest = pl.ds(pl.multiple_of((1 - t) * half, half), half)
                near = ROW * z + 2 - 2 * t + k + side - 2 * k * side
                ok = owner == seg(near * rows + lax.broadcasted_iota(jnp.int32, (1, rows), 1)).astype(f32)
                for h in range(HEADS):
                    cols = slice(h * head_dim, (h + 1) * head_dim)
                    keys = jnp.concatenate([kv[a, 0, low, cols], kv[b, 0, rest, cols]], axis=0)
                    values = jnp.concatenate([kv[a, 1, low, cols], kv[b, 1, rest, cols]], axis=0)
                    score = dot_t(qc_s[...][:, cols], keys) * half_scale
                    weight = jnp.where(ok, silu_of_twice(score), 0.0).astype(bf16)
                    part[g, :, cols] += dot(weight, values)
                return carry

            lax.fori_loop(0, 4, shard, 0)
            out3[at] = part[g].astype(bf16).reshape(lines, 2 * cr, width)
            return carry

        lax.fori_loop(0, depth // lines, one, 0)

        def send(d, c):
            for side in range(2):
                red(d, side).start()
            return c

        lax.fori_loop(1, depth, send, 0)
        red(0, 0).start()

    def red(d, side):
        src = out3.at[(z + d) % depth, pl.ds(side * cr, cr)]
        return remote(src, buf3.at[d], rz_send.at[side, d], rz_recv.at[d], (ROW * (z + d) + 2 * side + k) % n)

    def red_wait(d):
        return remote(out3.at[0, pl.ds(0, cr)], buf3.at[d], rz_send.at[0, d], rz_recv.at[d], partner).wait_recv()

    def only(side, f, *a):
        pl.when(p == side if side < 2 else r == side)(functools.partial(f, *a))

    def event(e):
        if e == 1:
            hop(B2, 0)
        if e == 2:
            hop(B2, 1)
            only(0, hop, B2, 2)
            for h in (0, 1):
                hop(B1, h)
                only(0, hop, B3, h)
        if e == 3:
            only(1, hop, B2, 2)
            only(1, send, 3, 0, 1)
            only(0, hop, B2, 3)
            only(0, send, 3, 0, PIECES)
        if e == 4:
            only(1, hop, B2, 3)
            for h in (2, 3):
                hop(B1, h)
                only(0, hop, B3, h)
            if depth > 1:
                only(1, c_round, 1)
            only(1, send, 3, 1, PIECES - 1)
        if e == 5:
            if depth > 2:
                only(1, c_round, 2)
            only(1, send, 3, PIECES - 1, PIECES)
            only(3, hop, B5, 0)
            only(3, hop, B5, 1)
        if e == 6:
            only(3, c_last)
            only(3, c_scores)
            only(2, c_last)
            only(2, c_scores)
            for h in (0, 1):
                only(2, hop, B5, h)
                only(1, hop, B3, h)
                only(0, hop, B4, h)
                only(0, hop, B5, h)
            late(1)
        if e == 7:
            late(0)

    def late(core):
        @pl.when(k == core)
        def _():
            for h in (2, 3):
                only(2, hop, B5, h)
                only(1, hop, B3, h)
                only(0, hop, B4, h)
                only(0, hop, B5, h)

    proj_table = {2: 1, 4: 2, 6: 3, 7: 4}
    att_table = {
        0: 1,
        1: 1 + SIB,
        2: 1 + 1,
        3: 1 + SIB + 1,
        4: 1 + 2,
        5: 1 + SIB + 2,
        6: 0,
        7: 1 + 3,
        8: 1 + 4,
        9: 1 + SIB + 3,
    }

    def live(t):
        return z >= jnp.minimum(t, 1) * (1 - p) + t // 3

    def one(e, carry):
        for at in range(8):

            @pl.when(e == at)
            def _():
                event(at)

        t = pick(e, proj_table)

        @pl.when((t > 0) & live(t) & ((t < 4) | (k == 0)))
        def _():
            end = t // 3
            one_at = (1 - end) * (1 - p) + end * (3 - p)
            two_at = (1 - end) * (2 - p) + end * (4 * (1 - k) + (3 - p) * k)
            one_off = (t + 1) % 2
            two_off = jnp.maximum(one_off, end * k)
            x1 = xb[one_at, pl.ds(pl.multiple_of(one_off * half, half), half)]
            x2 = xb[two_at, pl.ds(pl.multiple_of(two_off * half, half), half)]
            x = jnp.concatenate([x1, x2], axis=0)
            kv[t, 0] = project(x, 3)
            kv[t, 1] = project(x, 1)
            pl.when((t < 3) | ((t == 3) & (k == 1)))(lambda: swap_copy(t).start())
            pl.when((t == 3) & (k == 0))(lambda: swap_half(3).start())
            pl.when((t == 4) & (k == 0))(lambda: swap_half(4).start())

        a = pick(e, att_table) - 1
        ta = (a + SIB) % SIB
        side = (a + SIB) // SIB - 1

        @pl.when((a >= 0) & live(ta) & ((ta < 4) | (k == 0)) & ((ta > 0) | (side < 1) | (k == 1)))
        def _():
            pl.when((side == 1) & ((ta < 3) | (k == 0)))(lambda: swap_copy(ta).wait_recv())

            @pl.when((side == 1) & (ta == 3) & (k == 1))
            def _():
                swap_half(3).wait_recv()
                swap_half(4).wait_recv()

            attend(a)

        return carry

    lax.fori_loop(0, 10, one, 0)

    w_copies[4].wait()

    def take(d, c):
        red_wait(d)
        return c + buf3[d].astype(f32)

    def cand_rows():
        pl.when(p == 0)(lambda: red_wait(0))

        @pl.when(p == 1)
        def _():
            buf3[0] = out3[z, pl.ds(cr, cr)]

        cattn = lax.fori_loop(1, depth, take, buf3[0].astype(f32))
        return (layer_norm(cattn) * u_s[pl.ds(rows, cr)].astype(f32)).astype(bf16)

    def event_rows():
        return (layer_norm(acc[...]) * u_s[pl.ds(0, rows)].astype(f32)).astype(bf16)

    @pl.when(z < depth // 2)
    def _():
        out_ref[pl.ds(0, rows)] = (hist[...].astype(f32) + dot(event_rows(), w_out[...])).astype(bf16)
        out_ref[pl.ds(rows, cr)] = (cand[...].astype(f32) + dot(cand_rows(), w_out[...])).astype(bf16)

    @pl.when(z >= depth // 2)
    def _():
        y_c = cand_rows()
        both = dot(jnp.concatenate([event_rows(), y_c], axis=0), w_out[...])
        out_ref[pl.ds(0, rows)] = (hist[...].astype(f32) + both[:rows]).astype(bf16)
        out_ref[pl.ds(rows, cr)] = (cand[...].astype(f32) + both[rows:]).astype(bf16)

    for h in range(PIECES):
        for kind, src, dst, to, cond, _ in moves:
            if routed(kind, h):

                @pl.when(cond)
                def _():
                    x_copy(src, dst, h, kind, to).wait_send()

    for t, cond in ((0, (k == 0) | (p == 1)), (1, live(1)), (2, live(2)), (3, live(3) & (k == 1))):

        @pl.when(cond)
        def _():
            swap_copy(t).wait_send()

    @pl.when(live(3) & (k == 0))
    def _():
        swap_half(3).wait_send()
        swap_half(4).wait_send()

    pl.when(p == 0)(lambda: c_cross().wait_send())

    @pl.when(p == 1)
    def _():
        red(0, 0).wait_send()

        def left(d, c):
            pl.when(has_above & (z - d >= 0))(lambda: c_block(0, up_send.at[d], above).wait_send())
            pl.when(has_below & (z + d < depth))(lambda: c_block(0, down_send.at[d], below).wait_send())
            return c

        lax.fori_loop(0, depth, left, 0)

        def sums(d, c):
            for side in range(2):
                red(d, side).wait_send()
            return c

        lax.fori_loop(1, depth, sums, 0)


def hand_out(both, out_ref, cout_ref, sem):
    rows, cr = out_ref.shape[0], cout_ref.shape[0]
    parts = (pl.ds(0, rows), pl.ds(rows, cr))
    to = (out_ref, cout_ref)
    saves = [pltpu.make_async_copy(both.at[at], to[i], sem.at[i]) for i, at in enumerate(parts)]
    for c in saves:
        c.start()
    for c in saves:
        c.wait()


def per_device(n, history, candidates, lengths, cand_user, w_in, w_out):
    rows, width = history.shape
    cr = candidates.shape[0]
    depth = n // ROW
    users = cand_user[None, :]
    vmem = pl.BlockSpec(memory_space=pltpu.VMEM)
    dma = pltpu.SemaphoreType.DMA
    block = depth * 2 * cr
    group = min(block, 256)
    both = pl.pallas_call(
        functools.partial(kernel, n),
        out_shape=jax.ShapeDtypeStruct((rows + cr, width), bf16),
        in_specs=[pl.BlockSpec(memory_space=pltpu.HBM)] * 6,
        out_specs=vmem,
        scratch_shapes=[
            pltpu.SMEM(lengths.shape, jnp.int32),
            pltpu.VMEM((rows, width), bf16),
            pltpu.VMEM((cr, width), bf16),
            pltpu.VMEM((1, cr), jnp.int32),
            dma((4,)),
            pltpu.VMEM((4, width, width), bf16),
            pltpu.VMEM((width, width), bf16),
            pltpu.VMEM((rows, width), bf16),
            pltpu.VMEM((5, rows, width), bf16),
            pltpu.VMEM((SIB + 5, 2, rows, width), bf16),
            pltpu.VMEM((rows, width), bf16),
            pltpu.VMEM((rows + cr, width), bf16),
            pltpu.VMEM((rows, width), f32),
            pltpu.VMEM((cr, width + 128), bf16),
            pltpu.VMEM((depth, 2 * cr, width + 128), bf16),
            pltpu.VMEM((group, width), bf16),
            pltpu.VMEM((block // group, group, width), f32),
            pltpu.VMEM((depth, 2 * cr, width), bf16),
            pltpu.VMEM((depth, cr, width), bf16),
            dma((5,)),
            dma((8, PIECES)),
            dma((5, PIECES)),
            dma((5,)),
            dma((5,)),
            dma((1,)),
            dma((depth + 1,)),
            dma((depth,)),
            dma((depth,)),
            dma((2, depth)),
            dma((depth,)),
        ],
        compiler_params=pltpu.CompilerParams(
            collective_id=0, has_side_effects=True, vmem_limit_bytes=52 * 1024 * 1024
        ),
    )(*(pltpu.with_memory_space_constraint(x, pltpu.HBM) for x in (lengths, history, candidates, users, w_in, w_out)))
    hbm = pl.BlockSpec(memory_space=pl.ANY)
    return pl.pallas_call(
        hand_out,
        out_shape=(
            jax.ShapeDtypeStruct((rows, width), bf16),
            jax.ShapeDtypeStruct((cr, width), bf16),
        ),
        in_specs=[vmem],
        out_specs=(hbm, hbm),
        scratch_shapes=[dma((2,))],
        compiler_params=pltpu.CompilerParams(vmem_limit_bytes=2 * 1024 * 1024),
    )(both)


def solution(mesh):
    n = mesh.shape["seq"]
    placed = (
        P(("grp", "seq"), None),
        P(("grp", "seq"), None),
        P("grp"),
        P(("grp", "seq")),
        P(),
        P(),
    )
    return jax.shard_map(
        functools.partial(per_device, n),
        mesh=mesh,
        in_specs=placed,
        out_specs=(P(("grp", "seq"), None), P(("grp", "seq"), None)),
        check_vma=False,
    )
```

```python
import functools

import jax
import jax.numpy as jnp
from jax import lax
from jax.experimental import pallas as pl
from jax.experimental.pallas import tpu as pltpu
from jax.sharding import PartitionSpec as P

HEADS = 8
WIN = 8
PIECES = 4
ROW = 4
EARLY = 3
SIB = 6
B1, B2, B3, B4, B5 = 0, 1, 2, 3, 4

eps = 1e-06
bf16 = jnp.bfloat16
f32 = jnp.float32


def layer_norm(rows):
    centred = rows - jnp.mean(rows, axis=-1, keepdims=True)
    return centred * lax.rsqrt(jnp.mean(centred * centred, axis=-1, keepdims=True) + eps)


def silu_of_twice(half):
    return half + half * jnp.tanh(half)


def dot(a, b):
    return jnp.dot(a, b, preferred_element_type=f32)


def dot_t(a, b):
    return lax.dot_general(a, b, (((1,), (1,)), ((), ())), preferred_element_type=f32)


def pick(i, entries):
    out = 0
    for at, value in entries.items():
        out = out + value * (1 - jnp.minimum((i - at) * (i - at), 1))
    return out


def kernel(
    n,
    lengths_hbm,
    hist_hbm,
    cand_hbm,
    users_hbm,
    w_in_hbm,
    w_out_hbm,
    out_ref,
    lengths,
    hist,
    cand,
    users_row,
    in_sem,
    w_in,
    w_out,
    own,
    xb,
    kv,
    q_s,
    u_s,
    acc,
    cmsg,
    cbuf,
    qc_s,
    part,
    out3,
    buf3,
    w_sem,
    x_send,
    x_recv,
    kv_send,
    kv_recv,
    c_send,
    c_recv,
    up_send,
    down_send,
    rz_send,
    rz_recv,
):
    rows, width = hist.shape
    cr = cand.shape[0]
    head_dim = width // HEADS
    half_scale = 0.5 * head_dim ** (-0.5)
    depth = n // ROW
    s = lax.axis_index("seq")
    z = s // ROW
    r = s % ROW
    p = r // 2
    k = r % 2
    piece = rows // PIECES
    sibling = s + 1 - 2 * k
    partner = s + 2 - 4 * p
    above = (s + ROW) % n
    below = (s + n - ROW) % n
    has_above = z + 1 < depth
    has_below = z >= 1

    in_copies = [
        pltpu.make_async_copy(src, dst, in_sem.at[i])
        for i, (src, dst) in enumerate(
            (
                (hist_hbm.at[pl.ds(0, piece)], hist.at[pl.ds(0, piece)]),
                (hist_hbm.at[pl.ds(piece, rows - piece)], hist.at[pl.ds(piece, rows - piece)]),
                (cand_hbm, cand),
                (users_hbm, users_row),
                (lengths_hbm, lengths),
            )
        )
    ]
    for c in in_copies:
        c.start()
    w_copies = [
        pltpu.make_async_copy(
            w_in_hbm.at[0, :, pl.ds(c * width, width)], w_in.at[c], w_sem.at[c]
        )
        for c in range(4)
    ]
    w_copies.append(pltpu.make_async_copy(w_out_hbm.at[0], w_out, w_sem.at[4]))
    barrier = pltpu.get_barrier_semaphore()

    def greet(to):
        pl.semaphore_signal(barrier, inc=1, device_id={"seq": to}, device_id_type=pl.DeviceIdType.MESH)

    peers = (
        (None, sibling),
        (None, partner),
        (has_above, above),
        (has_below, below),
        (has_above & (r == 1), (s + 3) % n),
        (has_below & (r == 0), (s + n - 3) % n),
    )
    for cond, to in peers:
        if cond is None:
            greet(to)
        else:
            pl.when(cond)(functools.partial(greet, to))

    for c in (3, 1, 2, 0, 4):
        w_copies[c].start()
    def norm_rows(first, count):
        at = pl.ds(first, count)
        own[at] = layer_norm(hist[at].astype(f32)).astype(bf16)

    in_copies[0].wait()
    norm_rows(0, piece)

    @pl.when((p == 1) & (z == 0))
    def _():
        xb[B2] = jnp.zeros((rows, width), bf16)

    @pl.when((p == 1) & (k == 0) & (z == 1))
    def _():
        xb[B5] = jnp.zeros((rows, width), bf16)

    for c in in_copies[2:]:
        c.wait()

    eye = lax.broadcasted_iota(jnp.int32, (cr, cr), 0) == lax.broadcasted_iota(jnp.int32, (cr, cr), 1)
    column = jnp.sum(jnp.where(eye, users_row[...], 0), axis=1, keepdims=True)
    c_normed = layer_norm(cand[...].astype(f32)).astype(bf16)
    cmsg[:, :width] = c_normed
    cmsg[:, width:] = jnp.broadcast_to(column, (cr, 128)).astype(f32).astype(bf16)

    @pl.when(p == 1)
    def _():
        cbuf[z, pl.ds(cr, cr)] = cmsg[...]

    pl.semaphore_wait(barrier, sum(1 if cond is None else cond.astype(jnp.int32) for cond, _ in peers))

    def remote(src, dst, send, recv, to):
        return pltpu.make_async_remote_copy(
            src_ref=src,
            dst_ref=dst,
            send_sem=send,
            recv_sem=recv,
            device_id={"seq": to},
            device_id_type=pl.DeviceIdType.MESH,
        )

    def x_copy(src, dst, h, kind, to):
        at = pl.ds(h * piece, piece)
        return remote(src.at[at], xb.at[dst, at], x_send.at[kind, h], x_recv.at[dst, h], to)

    moves = (
        (0, own, B2, above, has_above, None),
        (1, own, B1, partner, p == 0, None),
        (2, xb.at[B2], B3, partner, has_below, B2),
        (3, xb.at[B2], B5, (s + 4) % n, has_below & has_above & (r == 3), None),
        (8, xb.at[B2], B5, (s + 3) % n, has_below & has_above & (r == 1), B2),
        (4, xb.at[B3], B4, above, has_below & has_above & (r == 0), B3),
        (5, xb.at[B5], B4, partner, (z >= 2) & (r == 3), B5),
        (7, xb.at[B3], B4, above, has_below & has_above & (r == 1), B3),
        (6, xb.at[B5], B5, sibling, (z >= 2) & (r == 3), B5),
    )
    arrives = {
        B1: p == 1,
        B2: has_below,
        B3: has_below,
        B4: (z >= 2) & (p == 0),
        B5: (z >= 2) & ((k == 0) | (p == 1)),
    }

    def c_cross():
        return remote(cmsg, cbuf.at[z, pl.ds(0, cr)], c_send.at[0], c_recv.at[depth], partner)

    def c_block(block, send, to):
        return remote(cbuf.at[block], cbuf.at[block], send, c_recv.at[block], to)

    def send(which, first, last, also=None):
        kind, src, dst, to, cond, _ = moves[which]

        @pl.when(cond if also is None else cond & also)
        def _():
            for h in range(first, last):
                x_copy(src, dst, h, kind, to).start()

    def own_out(h):
        send(0, h, h + 1, None if h < EARLY else p == 0)
        send(1, h, h + 1)

    @pl.when(p == 0)
    def _():
        c_cross().start()

    own_out(0)
    in_copies[1].wait()
    norm_rows(piece, rows - piece)
    for h in range(1, PIECES):
        own_out(h)
    normed = own[...]

    def routed(kind, h):
        return {5: h < PIECES // 2, 7: h >= PIECES // 2}.get(kind, True)

    def hop(buf, h):
        at = pl.ds(h * piece, piece)

        @pl.when(arrives[buf])
        def _():
            pltpu.make_async_copy(hist.at[at], xb.at[buf, at], x_recv.at[buf, h]).wait()
            for kind, src, dst, to, cond, source in moves:
                if source == buf and routed(kind, h):

                    @pl.when(cond)
                    def _():
                        x_copy(src, dst, h, kind, to).start()

    ends = []
    total = jnp.int32(0)
    for j in range(lengths.shape[0]):
        total = total + lengths[j]
        ends.append(total)

    def seg(pos):
        out = jnp.zeros(pos.shape, jnp.int32)
        for e in ends:
            out = out + (pos >= e).astype(jnp.int32)
        return out

    q_pos = s * rows + lax.broadcasted_iota(jnp.int32, (rows, 1), 0)
    q_seg = seg(q_pos)

    def project(normed, block):
        return silu_of_twice(dot(normed, w_in[block]) * 0.5).astype(bf16)

    half = rows // 2
    low = pl.ds(0, half)
    high = pl.ds(half, half)

    def swap_copy(t):
        return remote(kv.at[t], kv.at[SIB + t], kv_send.at[t], kv_recv.at[t], sibling)

    def swap_half(t):
        to = low if t == 3 else high
        return remote(kv.at[t, :, low], kv.at[SIB + 3, :, to], kv_send.at[t], kv_recv.at[t], sibling)

    def bases(t, side):
        kk = k + side - 2 * k * side
        first = ROW * (z - 1 + p) + kk
        second = ROW * (z - 1) + 2 + kk
        late = ROW * (z - 2 + p) + 2 - 2 * p + kk
        lone = ROW * (z - 2) + 1 + 2 * p
        mine = s + side * (1 - 2 * k)
        whole = k * (1 - side) + side
        h = half
        a = pick(t, {0: mine * rows, 1: first * rows, 2: first * rows + h, 3: late * rows, 4: late * rows + h})
        b = pick(
            t,
            {
                0: mine * rows + h,
                1: second * rows,
                2: second * rows + h,
                3: (1 - whole) * lone * rows + whole * (late * rows + h),
                4: lone * rows + h,
            },
        )
        return a, b

    def attend(a):
        start, later = bases(a % SIB, a // SIB)
        lane = lax.broadcasted_iota(jnp.int32, (1, rows), 1)
        k_pos = jnp.where(lane < half, start + lane, later + lane - half)
        ok = (k_pos <= q_pos) & (q_pos - k_pos < (WIN - 1) * rows) & (seg(k_pos) == q_seg)
        for h in range(HEADS):
            cols = slice(h * head_dim, (h + 1) * head_dim)
            score = dot_t(q_s[:, cols], kv[a, 0, :, cols]) * half_scale
            weight = jnp.where(ok, silu_of_twice(score), 0.0).astype(bf16)
            acc[:, cols] += dot(weight, kv[a, 1, :, cols])

    w_copies[3].wait()
    kv[0, 0] = project(normed, 3)
    w_copies[1].wait()
    kv[0, 1] = project(normed, 1)

    @pl.when((k == 0) | (p == 1))
    def _():
        swap_copy(0).start()

    def c_down(d):
        high = jnp.minimum(z + d, depth - 1)

        @pl.when(z + d < depth)
        def _():
            c_block(high, down_send.at[d], below).wait_recv()
            pl.when(has_below)(lambda: c_block(high, down_send.at[d], below).start())

    def c_up(d):
        low = jnp.maximum(z - d, 0)

        @pl.when(z - d >= 0)
        def _():
            c_block(low, up_send.at[d], above).wait_recv()
            pl.when(has_above)(lambda: c_block(low, up_send.at[d], above).start())

    def c_first():
        c_cross().wait_recv()
        pl.when(has_below)(lambda: c_block(z, down_send.at[0], below).start())
        pl.when(has_above)(lambda: c_block(z, up_send.at[0], above).start())

    w_copies[2].wait()
    q_s[...] = project(normed, 2)
    w_copies[0].wait()
    u_s[...] = project(jnp.concatenate([normed, c_normed], axis=0), 0)
    acc[...] = jnp.zeros_like(acc)
    pl.when(p == 1)(c_first)
    send(0, EARLY, EARLY + 1, p == 1)

    group = part.shape[1]
    lines = group // (2 * cr)

    def c_last():
        def rest(d, carry):
            c_down(d)
            c_up(d)
            return carry

        lax.fori_loop(3, depth, rest, 0)

    def c_scores():
        pl.when(k == 0)(lambda: swap_copy(0).wait_recv())

        def one(g, carry):
            at = pl.ds(pl.multiple_of(g * lines, lines), lines)
            qc_s[...] = project(cbuf[at, :, :width].reshape(group, width), 2)
            owner = cbuf[at, :, width:].reshape(group, 128)[:, :1].astype(f32)
            part[g] = jnp.zeros((group, width), f32)

            def shard(i, carry):
                for at in (2, 3):
                    pl.when((r == 3) & (g == 0) & (i == 2 * at - 3))(functools.partial(hop, B5, at))
                t = i // 2
                side = i % 2
                a = t + side * SIB
                b = 2 * t + side * SIB
                rest = pl.ds(pl.multiple_of((1 - t) * half, half), half)
                near = ROW * z + 2 - 2 * t + k + side - 2 * k * side
                ok = owner == seg(near * rows + lax.broadcasted_iota(jnp.int32, (1, rows), 1)).astype(f32)
                for h in range(HEADS):
                    cols = slice(h * head_dim, (h + 1) * head_dim)
                    keys = jnp.concatenate([kv[a, 0, low, cols], kv[b, 0, rest, cols]], axis=0)
                    values = jnp.concatenate([kv[a, 1, low, cols], kv[b, 1, rest, cols]], axis=0)
                    score = dot_t(qc_s[...][:, cols], keys) * half_scale
                    weight = jnp.where(ok, silu_of_twice(score), 0.0).astype(bf16)
                    part[g, :, cols] += dot(weight, values)
                return carry

            lax.fori_loop(0, 4, shard, 0)
            out3[at] = part[g].astype(bf16).reshape(lines, 2 * cr, width)
            return carry

        lax.fori_loop(0, depth // lines, one, 0)

        def send(d, c):
            for side in range(2):
                red(d, side).start()
            return c

        lax.fori_loop(1, depth, send, 0)
        red(0, 0).start()

    def red(d, side):
        src = out3.at[(z + d) % depth, pl.ds(side * cr, cr)]
        return remote(src, buf3.at[d], rz_send.at[side, d], rz_recv.at[d], (ROW * (z + d) + 2 * side + k) % n)

    def red_wait(d):
        return remote(out3.at[0, pl.ds(0, cr)], buf3.at[d], rz_send.at[0, d], rz_recv.at[d], partner).wait_recv()

    def only(side, f, *a):
        pl.when(p == side if side < 2 else r == side)(functools.partial(f, *a))

    def event(e):
        if e == 1:
            hop(B2, 0)
        if e == 2:
            hop(B2, 1)
            only(0, hop, B2, 2)
            for h in (0, 1):
                hop(B1, h)
                only(0, hop, B3, h)
        if e == 3:
            only(1, hop, B2, 2)
            only(1, send, 3, 0, 1)
            only(0, hop, B2, 3)
        if e == 4:
            if depth > 1:
                only(1, c_down, 1)
                only(1, c_up, 1)
            only(1, hop, B2, 3)
            for h in (2, 3):
                hop(B1, h)
                only(0, hop, B3, h)
            only(1, send, 3, 1, PIECES - 1)
        if e == 5:
            if depth > 2:
                only(1, c_down, 2)
                only(1, c_up, 2)
            only(1, send, 3, PIECES - 1, PIECES)
            only(3, hop, B5, 0)
            only(3, hop, B5, 1)
        if e == 6:
            @pl.when(p == 1)
            def _():
                c_last()
                c_scores()

            for h in (0, 1):
                only(2, hop, B5, h)
                only(1, hop, B3, h)
                only(0, hop, B4, h)
                only(0, hop, B5, h)
            late(1)
        if e == 7:
            late(0)

    def late(core):
        @pl.when(k == core)
        def _():
            for h in (2, 3):
                only(2, hop, B5, h)
                only(1, hop, B3, h)
                only(0, hop, B4, h)
                only(0, hop, B5, h)

    proj_table = {2: 1, 4: 2, 6: 3, 7: 4}
    att_table = {
        0: 1,
        1: 1 + SIB,
        2: 1 + 1,
        3: 1 + SIB + 1,
        4: 1 + 2,
        5: 1 + SIB + 2,
        6: 0,
        7: 1 + 3,
        8: 1 + 4,
        9: 1 + SIB + 3,
    }

    def live(t):
        return z >= jnp.minimum(t, 1) * (1 - p) + t // 3

    def one(e, carry):
        for at in range(8):

            @pl.when(e == at)
            def _():
                event(at)

        t = pick(e, proj_table)

        @pl.when((t > 0) & live(t) & ((t < 4) | (k == 0)))
        def _():
            end = t // 3
            one_at = (1 - end) * (1 - p) + end * (3 - p)
            two_at = (1 - end) * (2 - p) + end * (4 * (1 - k) + (3 - p) * k)
            one_off = (t + 1) % 2
            two_off = jnp.maximum(one_off, end * k)
            x1 = xb[one_at, pl.ds(pl.multiple_of(one_off * half, half), half)]
            x2 = xb[two_at, pl.ds(pl.multiple_of(two_off * half, half), half)]
            x = jnp.concatenate([x1, x2], axis=0)
            kv[t, 0] = project(x, 3)
            kv[t, 1] = project(x, 1)
            pl.when((t < 3) | ((t == 3) & (k == 1)))(lambda: swap_copy(t).start())
            pl.when((t == 3) & (k == 0))(lambda: swap_half(3).start())
            pl.when((t == 4) & (k == 0))(lambda: swap_half(4).start())

        a = pick(e, att_table) - 1
        ta = (a + SIB) % SIB
        side = (a + SIB) // SIB - 1

        @pl.when((a >= 0) & live(ta) & ((ta < 4) | (k == 0)) & ((ta > 0) | (side < 1) | (k == 1)))
        def _():
            pl.when((side == 1) & ((ta < 3) | (k == 0)))(lambda: swap_copy(ta).wait_recv())

            @pl.when((side == 1) & (ta == 3) & (k == 1))
            def _():
                swap_half(3).wait_recv()
                swap_half(4).wait_recv()

            attend(a)

        return carry

    lax.fori_loop(0, 10, one, 0)

    w_copies[4].wait()

    def take(d, c):
        red_wait(d)
        return c + buf3[d].astype(f32)

    def cand_rows():
        pl.when(p == 0)(lambda: red_wait(0))

        @pl.when(p == 1)
        def _():
            buf3[0] = out3[z, pl.ds(cr, cr)]

        cattn = lax.fori_loop(1, depth, take, buf3[0].astype(f32))
        return (layer_norm(cattn) * u_s[pl.ds(rows, cr)].astype(f32)).astype(bf16)

    def event_rows():
        return (layer_norm(acc[...]) * u_s[pl.ds(0, rows)].astype(f32)).astype(bf16)

    @pl.when(has_above)
    def _():
        out_ref[pl.ds(0, rows)] = (hist[...].astype(f32) + dot(event_rows(), w_out[...])).astype(bf16)

    for h in range(PIECES):
        for kind, src, dst, to, cond, _ in moves:
            if routed(kind, h):

                @pl.when(cond)
                def _():
                    x_copy(src, dst, h, kind, to).wait_send()

    for t, cond in ((0, (k == 0) | (p == 1)), (1, live(1)), (2, live(2)), (3, live(3) & (k == 1))):

        @pl.when(cond)
        def _():
            swap_copy(t).wait_send()

    @pl.when(live(3) & (k == 0))
    def _():
        swap_half(3).wait_send()
        swap_half(4).wait_send()

    pl.when(p == 0)(lambda: c_cross().wait_send())

    @pl.when(p == 1)
    def _():
        def left(d, c):
            pl.when(has_above & (z - d >= 0))(lambda: c_block(0, up_send.at[d], above).wait_send())
            pl.when(has_below & (z + d < depth))(lambda: c_block(0, down_send.at[d], below).wait_send())
            return c

        lax.fori_loop(0, depth, left, 0)

    @pl.when(has_above)
    def _():
        out_ref[pl.ds(rows, cr)] = (cand[...].astype(f32) + dot(cand_rows(), w_out[...])).astype(bf16)

    @pl.when(z + 1 == depth)
    def _():
        y_c = cand_rows()
        both = dot(jnp.concatenate([event_rows(), y_c], axis=0), w_out[...])
        out_ref[pl.ds(0, rows)] = (hist[...].astype(f32) + both[:rows]).astype(bf16)
        out_ref[pl.ds(rows, cr)] = (cand[...].astype(f32) + both[rows:]).astype(bf16)

    @pl.when(p == 1)
    def _():
        red(0, 0).wait_send()

        def sums(d, c):
            for side in range(2):
                red(d, side).wait_send()
            return c

        lax.fori_loop(1, depth, sums, 0)


def hand_out(both, out_ref, cout_ref, sem):
    rows, cr = out_ref.shape[0], cout_ref.shape[0]
    parts = (pl.ds(0, rows), pl.ds(rows, cr))
    to = (out_ref, cout_ref)
    saves = [pltpu.make_async_copy(both.at[at], to[i], sem.at[i]) for i, at in enumerate(parts)]
    for c in saves:
        c.start()
    for c in saves:
        c.wait()


def per_device(n, history, candidates, lengths, cand_user, w_in, w_out):
    rows, width = history.shape
    cr = candidates.shape[0]
    depth = n // ROW
    users = cand_user[None, :]
    vmem = pl.BlockSpec(memory_space=pltpu.VMEM)
    dma = pltpu.SemaphoreType.DMA
    block = depth * 2 * cr
    group = min(block, 256)
    both = pl.pallas_call(
        functools.partial(kernel, n),
        out_shape=jax.ShapeDtypeStruct((rows + cr, width), bf16),
        in_specs=[pl.BlockSpec(memory_space=pltpu.HBM)] * 6,
        out_specs=vmem,
        scratch_shapes=[
            pltpu.SMEM(lengths.shape, jnp.int32),
            pltpu.VMEM((rows, width), bf16),
            pltpu.VMEM((cr, width), bf16),
            pltpu.VMEM((1, cr), jnp.int32),
            dma((5,)),
            pltpu.VMEM((4, width, width), bf16),
            pltpu.VMEM((width, width), bf16),
            pltpu.VMEM((rows, width), bf16),
            pltpu.VMEM((5, rows, width), bf16),
            pltpu.VMEM((SIB + 5, 2, rows, width), bf16),
            pltpu.VMEM((rows, width), bf16),
            pltpu.VMEM((rows + cr, width), bf16),
            pltpu.VMEM((rows, width), f32),
            pltpu.VMEM((cr, width + 128), bf16),
            pltpu.VMEM((depth, 2 * cr, width + 128), bf16),
            pltpu.VMEM((group, width), bf16),
            pltpu.VMEM((block // group, group, width), f32),
            pltpu.VMEM((depth, 2 * cr, width), bf16),
            pltpu.VMEM((depth, cr, width), bf16),
            dma((5,)),
            dma((9, PIECES)),
            dma((5, PIECES)),
            dma((5,)),
            dma((5,)),
            dma((1,)),
            dma((depth + 1,)),
            dma((depth,)),
            dma((depth,)),
            dma((2, depth)),
            dma((depth,)),
        ],
        compiler_params=pltpu.CompilerParams(
            collective_id=0, has_side_effects=True, vmem_limit_bytes=52 * 1024 * 1024
        ),
    )(*(pltpu.with_memory_space_constraint(x, pltpu.HBM) for x in (lengths, history, candidates, users, w_in, w_out)))
    hbm = pl.BlockSpec(memory_space=pl.ANY)
    return pl.pallas_call(
        hand_out,
        out_shape=(
            jax.ShapeDtypeStruct((rows, width), bf16),
            jax.ShapeDtypeStruct((cr, width), bf16),
        ),
        in_specs=[vmem],
        out_specs=(hbm, hbm),
        scratch_shapes=[dma((2,))],
        compiler_params=pltpu.CompilerParams(vmem_limit_bytes=2 * 1024 * 1024),
    )(both)


def solution(mesh):
    n = mesh.shape["seq"]
    placed = (
        P(("grp", "seq"), None),
        P(("grp", "seq"), None),
        P("grp"),
        P(("grp", "seq")),
        P(),
        P(),
    )
    return jax.shard_map(
        functools.partial(per_device, n),
        mesh=mesh,
        in_specs=placed,
        out_specs=(P(("grp", "seq"), None), P(("grp", "seq"), None)),
        check_vma=False,
    )
```

```python
import functools

import jax
import jax.numpy as jnp
from jax import lax
from jax.experimental import pallas as pl
from jax.experimental.pallas import tpu as pltpu
from jax.sharding import PartitionSpec as P

HEADS = 8
WIN = 8
PIECES = 4
ROW = 4
EARLY = 3
SIB = 6
B1, B2, B3, B4, B5 = 0, 1, 2, 3, 4

eps = 1e-06
bf16 = jnp.bfloat16
f32 = jnp.float32


def layer_norm(rows):
    centred = rows - jnp.mean(rows, axis=-1, keepdims=True)
    return centred * lax.rsqrt(jnp.mean(centred * centred, axis=-1, keepdims=True) + eps)


def silu_of_twice(half):
    return half + half * jnp.tanh(half)


def dot(a, b):
    return jnp.dot(a, b, preferred_element_type=f32)


def dot_t(a, b):
    return lax.dot_general(a, b, (((1,), (1,)), ((), ())), preferred_element_type=f32)


def pick(i, entries):
    out = 0
    for at, value in entries.items():
        out = out + value * (1 - jnp.minimum((i - at) * (i - at), 1))
    return out


def kernel(
    n,
    lengths_hbm,
    hist_hbm,
    cand_hbm,
    users_hbm,
    w_in_hbm,
    w_out_hbm,
    out_ref,
    lengths,
    hist,
    cand,
    users_row,
    in_sem,
    w_in,
    w_out,
    own,
    xb,
    kv,
    q_s,
    u_s,
    acc,
    cmsg,
    cbuf,
    qc_s,
    part,
    out3,
    buf3,
    w_sem,
    x_send,
    x_recv,
    kv_send,
    kv_recv,
    c_send,
    c_recv,
    up_send,
    down_send,
    rz_send,
    rz_recv,
):
    rows, width = hist.shape
    cr = cand.shape[0]
    head_dim = width // HEADS
    half_scale = 0.5 * head_dim ** (-0.5)
    depth = n // ROW
    s = lax.axis_index("seq")
    z = s // ROW
    r = s % ROW
    p = r // 2
    k = r % 2
    piece = rows // PIECES
    sibling = s + 1 - 2 * k
    partner = s + 2 - 4 * p
    above = (s + ROW) % n
    below = (s + n - ROW) % n
    has_above = z + 1 < depth
    has_below = z >= 1

    in_copies = [
        pltpu.make_async_copy(src, dst, in_sem.at[i])
        for i, (src, dst) in enumerate(
            (
                (hist_hbm.at[pl.ds(0, piece)], hist.at[pl.ds(0, piece)]),
                (hist_hbm.at[pl.ds(piece, rows - piece)], hist.at[pl.ds(piece, rows - piece)]),
                (cand_hbm, cand),
                (users_hbm, users_row),
                (lengths_hbm, lengths),
            )
        )
    ]
    for c in in_copies:
        c.start()
    w_copies = [
        pltpu.make_async_copy(
            w_in_hbm.at[0, :, pl.ds(c * width, width)], w_in.at[c], w_sem.at[c]
        )
        for c in range(4)
    ]
    w_copies.append(pltpu.make_async_copy(w_out_hbm.at[0], w_out, w_sem.at[4]))
    barrier = pltpu.get_barrier_semaphore()

    def greet(to):
        pl.semaphore_signal(barrier, inc=1, device_id={"seq": to}, device_id_type=pl.DeviceIdType.MESH)

    peers = (
        (None, sibling),
        (None, partner),
        (has_above, above),
        (has_below, below),
        (has_above & (r == 1), (s + 3) % n),
        (has_below & (r == 0), (s + n - 3) % n),
    )
    for cond, to in peers:
        if cond is None:
            greet(to)
        else:
            pl.when(cond)(functools.partial(greet, to))

    for c in (3, 1, 2, 0, 4):
        w_copies[c].start()
    def norm_rows(first, count):
        at = pl.ds(first, count)
        own[at] = layer_norm(hist[at].astype(f32)).astype(bf16)

    in_copies[0].wait()
    norm_rows(0, piece)

    @pl.when((p == 1) & (z == 0))
    def _():
        xb[B2] = jnp.zeros((rows, width), bf16)

    @pl.when((p == 1) & (k == 0) & (z == 1))
    def _():
        xb[B5] = jnp.zeros((rows, width), bf16)

    for c in in_copies[2:]:
        c.wait()

    eye = lax.broadcasted_iota(jnp.int32, (cr, cr), 0) == lax.broadcasted_iota(jnp.int32, (cr, cr), 1)
    column = jnp.sum(jnp.where(eye, users_row[...], 0), axis=1, keepdims=True)
    c_normed = layer_norm(cand[...].astype(f32)).astype(bf16)
    cmsg[:, :width] = c_normed
    cmsg[:, width:] = jnp.broadcast_to(column, (cr, 128)).astype(f32).astype(bf16)

    @pl.when(p == 1)
    def _():
        cbuf[z, pl.ds(cr, cr)] = cmsg[...]

    pl.semaphore_wait(barrier, sum(1 if cond is None else cond.astype(jnp.int32) for cond, _ in peers))

    def remote(src, dst, send, recv, to):
        return pltpu.make_async_remote_copy(
            src_ref=src,
            dst_ref=dst,
            send_sem=send,
            recv_sem=recv,
            device_id={"seq": to},
            device_id_type=pl.DeviceIdType.MESH,
        )

    def x_copy(src, dst, h, kind, to):
        at = pl.ds(h * piece, piece)
        return remote(src.at[at], xb.at[dst, at], x_send.at[kind, h], x_recv.at[dst, h], to)

    moves = (
        (0, own, B2, above, has_above, None),
        (1, own, B1, partner, p == 0, None),
        (2, xb.at[B2], B3, partner, has_below, B2),
        (3, xb.at[B2], B5, (s + 4) % n, has_below & has_above & (r == 3), None),
        (8, xb.at[B2], B5, (s + 3) % n, has_below & has_above & (r == 1), B2),
        (4, xb.at[B3], B4, above, has_below & has_above & (r == 0), B3),
        (5, xb.at[B5], B4, partner, (z >= 2) & (r == 3), B5),
        (7, xb.at[B3], B4, above, has_below & has_above & (r == 1), B3),
        (6, xb.at[B5], B5, sibling, (z >= 2) & (r == 3), B5),
    )
    arrives = {
        B1: p == 1,
        B2: has_below,
        B3: has_below,
        B4: (z >= 2) & (p == 0),
        B5: (z >= 2) & ((k == 0) | (p == 1)),
    }

    def c_cross():
        return remote(cmsg, cbuf.at[z, pl.ds(0, cr)], c_send.at[0], c_recv.at[depth], partner)

    def c_block(block, send, to):
        return remote(cbuf.at[block], cbuf.at[block], send, c_recv.at[block], to)

    def send(which, first, last, also=None):
        kind, src, dst, to, cond, _ = moves[which]

        @pl.when(cond if also is None else cond & also)
        def _():
            for h in range(first, last):
                x_copy(src, dst, h, kind, to).start()

    def own_out(h):
        send(0, h, h + 1, None if h < EARLY else p == 0)
        send(1, h, h + 1)

    @pl.when(p == 0)
    def _():
        c_cross().start()

    own_out(0)
    in_copies[1].wait()
    norm_rows(piece, rows - piece)
    for h in range(1, PIECES):
        own_out(h)
    normed = own[...]

    def routed(kind, h):
        return {5: h < PIECES // 2, 7: h >= PIECES // 2}.get(kind, True)

    def hop(buf, h):
        at = pl.ds(h * piece, piece)

        @pl.when(arrives[buf])
        def _():
            pltpu.make_async_copy(hist.at[at], xb.at[buf, at], x_recv.at[buf, h]).wait()
            for kind, src, dst, to, cond, source in moves:
                if source == buf and routed(kind, h):

                    @pl.when(cond)
                    def _():
                        x_copy(src, dst, h, kind, to).start()

    ends = []
    total = jnp.int32(0)
    for j in range(lengths.shape[0]):
        total = total + lengths[j]
        ends.append(total)

    def seg(pos):
        out = jnp.zeros(pos.shape, jnp.int32)
        for e in ends:
            out = out + (pos >= e).astype(jnp.int32)
        return out

    q_pos = s * rows + lax.broadcasted_iota(jnp.int32, (rows, 1), 0)
    q_seg = seg(q_pos)

    def project(normed, block):
        return silu_of_twice(dot(normed, w_in[block]) * 0.5).astype(bf16)

    half = rows // 2
    low = pl.ds(0, half)
    high = pl.ds(half, half)

    def swap_copy(t):
        return remote(kv.at[t], kv.at[SIB + t], kv_send.at[t], kv_recv.at[t], sibling)

    def swap_half(t):
        to = low if t == 3 else high
        return remote(kv.at[t, :, low], kv.at[SIB + 3, :, to], kv_send.at[t], kv_recv.at[t], sibling)

    def bases(t, side):
        kk = k + side - 2 * k * side
        first = ROW * (z - 1 + p) + kk
        second = ROW * (z - 1) + 2 + kk
        late = ROW * (z - 2 + p) + 2 - 2 * p + kk
        lone = ROW * (z - 2) + 1 + 2 * p
        mine = s + side * (1 - 2 * k)
        whole = k * (1 - side) + side
        h = half
        a = pick(t, {0: mine * rows, 1: first * rows, 2: first * rows + h, 3: late * rows, 4: late * rows + h})
        b = pick(
            t,
            {
                0: mine * rows + h,
                1: second * rows,
                2: second * rows + h,
                3: (1 - whole) * lone * rows + whole * (late * rows + h),
                4: lone * rows + h,
            },
        )
        return a, b

    def attend(a):
        start, later = bases(a % SIB, a // SIB)
        lane = lax.broadcasted_iota(jnp.int32, (1, rows), 1)
        k_pos = jnp.where(lane < half, start + lane, later + lane - half)
        ok = (k_pos <= q_pos) & (q_pos - k_pos < (WIN - 1) * rows) & (seg(k_pos) == q_seg)
        for h in range(HEADS):
            cols = slice(h * head_dim, (h + 1) * head_dim)
            score = dot_t(q_s[:, cols], kv[a, 0, :, cols]) * half_scale
            weight = jnp.where(ok, silu_of_twice(score), 0.0).astype(bf16)
            acc[:, cols] += dot(weight, kv[a, 1, :, cols])

    w_copies[3].wait()
    kv[0, 0] = project(normed, 3)
    w_copies[1].wait()
    kv[0, 1] = project(normed, 1)

    @pl.when((k == 0) | (p == 1))
    def _():
        swap_copy(0).start()

    def c_down(d):
        high = jnp.minimum(z + d, depth - 1)

        @pl.when(z + d < depth)
        def _():
            c_block(high, down_send.at[d], below).wait_recv()
            pl.when(has_below)(lambda: c_block(high, down_send.at[d], below).start())

    def c_up(d):
        low = jnp.maximum(z - d, 0)

        @pl.when(z - d >= 0)
        def _():
            c_block(low, up_send.at[d], above).wait_recv()
            pl.when(has_above)(lambda: c_block(low, up_send.at[d], above).start())

    def c_first():
        c_cross().wait_recv()
        pl.when(has_below)(lambda: c_block(z, down_send.at[0], below).start())
        pl.when(has_above)(lambda: c_block(z, up_send.at[0], above).start())

    w_copies[2].wait()
    q_s[...] = project(normed, 2)
    w_copies[0].wait()
    u_s[...] = project(jnp.concatenate([normed, c_normed], axis=0), 0)
    acc[...] = jnp.zeros_like(acc)
    pl.when(p == 1)(c_first)
    send(0, EARLY, EARLY + 1, p == 1)

    group = part.shape[1]
    lines = group // (2 * cr)

    def c_last():
        def rest(d, carry):
            c_down(d)
            c_up(d)
            return carry

        lax.fori_loop(3, depth, rest, 0)

    def c_scores():
        pl.when(k == 0)(lambda: swap_copy(0).wait_recv())

        def one(g, carry):
            at = pl.ds(pl.multiple_of(g * lines, lines), lines)
            qc_s[...] = project(cbuf[at, :, :width].reshape(group, width), 2)
            owner = cbuf[at, :, width:].reshape(group, 128)[:, :1].astype(f32)
            part[g] = jnp.zeros((group, width), f32)

            def shard(i, carry):
                if i % 2:
                    pl.when((r == 3) & (g == 0))(functools.partial(hop, B5, (i + 3) // 2))
                t = i // 2
                side = i % 2
                a = t + side * SIB
                b = 2 * t + side * SIB
                rest = pl.ds((1 - t) * half, half)
                near = ROW * z + 2 - 2 * t + k + side - 2 * k * side
                ok = owner == seg(near * rows + lax.broadcasted_iota(jnp.int32, (1, rows), 1)).astype(f32)
                for h in range(HEADS):
                    cols = slice(h * head_dim, (h + 1) * head_dim)
                    keys = jnp.concatenate([kv[a, 0, low, cols], kv[b, 0, rest, cols]], axis=0)
                    values = jnp.concatenate([kv[a, 1, low, cols], kv[b, 1, rest, cols]], axis=0)
                    score = dot_t(qc_s[...][:, cols], keys) * half_scale
                    weight = jnp.where(ok, silu_of_twice(score), 0.0).astype(bf16)
                    part[g, :, cols] += dot(weight, values)
                return carry

            for i in range(4):
                shard(i, 0)
            out3[at] = part[g].astype(bf16).reshape(lines, 2 * cr, width)
            return carry

        lax.fori_loop(0, depth // lines, one, 0)

        def send(d, c):
            for side in range(2):
                red(d, side).start()
            return c

        lax.fori_loop(1, depth, send, 0)
        red(0, 0).start()

    def red(d, side):
        src = out3.at[(z + d) % depth, pl.ds(side * cr, cr)]
        return remote(src, buf3.at[d], rz_send.at[side, d], rz_recv.at[d], (ROW * (z + d) + 2 * side + k) % n)

    def red_wait(d):
        return remote(out3.at[0, pl.ds(0, cr)], buf3.at[d], rz_send.at[0, d], rz_recv.at[d], partner).wait_recv()

    def only(side, f, *a):
        pl.when(p == side if side < 2 else r == side)(functools.partial(f, *a))

    def event(e):
        if e == 1:
            hop(B2, 0)
        if e == 2:
            hop(B2, 1)
            only(0, hop, B2, 2)
            for h in (0, 1):
                hop(B1, h)
                only(0, hop, B3, h)
        if e == 3:
            only(1, hop, B2, 2)
            only(1, send, 3, 0, 1)
            only(0, hop, B2, 3)
        if e == 4:
            if depth > 1:
                only(1, c_down, 1)
                only(1, c_up, 1)
            only(1, hop, B2, 3)
            for h in (2, 3):
                hop(B1, h)
                only(0, hop, B3, h)
            only(1, send, 3, 1, PIECES - 1)
        if e == 5:
            if depth > 2:
                only(1, c_down, 2)
                only(1, c_up, 2)
            only(1, send, 3, PIECES - 1, PIECES)
            only(3, hop, B5, 0)
            only(3, hop, B5, 1)
        if e == 6:
            @pl.when(p == 1)
            def _():
                c_last()
                c_scores()

            for h in (0, 1):
                only(2, hop, B5, h)
                only(1, hop, B3, h)
                only(0, hop, B4, h)
                only(0, hop, B5, h)
            late(1)
        if e == 7:
            late(0)

    def late(core):
        @pl.when(k == core)
        def _():
            for h in (2, 3):
                only(2, hop, B5, h)
                only(1, hop, B3, h)
                only(0, hop, B4, h)
                only(0, hop, B5, h)

    proj_table = {2: 1, 4: 2, 6: 3, 7: 4}
    att_table = {
        0: 1,
        1: 1 + SIB,
        2: 1 + 1,
        3: 1 + SIB + 1,
        4: 1 + 2,
        5: 1 + SIB + 2,
        6: 0,
        7: 1 + 3,
        8: 1 + 4,
        9: 1 + SIB + 3,
    }

    def live(t):
        return z >= jnp.minimum(t, 1) * (1 - p) + t // 3

    def one(e, carry):
        for at in range(8):

            @pl.when(e == at)
            def _():
                event(at)

        t = pick(e, proj_table)

        @pl.when((t > 0) & live(t) & ((t < 4) | (k == 0)))
        def _():
            end = t // 3
            one_at = (1 - end) * (1 - p) + end * (3 - p)
            two_at = (1 - end) * (2 - p) + end * (4 * (1 - k) + (3 - p) * k)
            one_off = (t + 1) % 2
            two_off = jnp.maximum(one_off, end * k)
            x1 = xb[one_at, pl.ds(pl.multiple_of(one_off * half, half), half)]
            x2 = xb[two_at, pl.ds(pl.multiple_of(two_off * half, half), half)]
            x = jnp.concatenate([x1, x2], axis=0)
            kv[t, 0] = project(x, 3)
            kv[t, 1] = project(x, 1)
            pl.when((t < 3) | ((t == 3) & (k == 1)))(lambda: swap_copy(t).start())
            pl.when((t == 3) & (k == 0))(lambda: swap_half(3).start())
            pl.when((t == 4) & (k == 0))(lambda: swap_half(4).start())

        a = pick(e, att_table) - 1
        ta = (a + SIB) % SIB
        side = (a + SIB) // SIB - 1

        @pl.when((a >= 0) & live(ta) & ((ta < 4) | (k == 0)) & ((ta > 0) | (side < 1) | (k == 1)))
        def _():
            pl.when((side == 1) & ((ta < 3) | (k == 0)))(lambda: swap_copy(ta).wait_recv())

            @pl.when((side == 1) & (ta == 3) & (k == 1))
            def _():
                swap_half(3).wait_recv()
                swap_half(4).wait_recv()

            attend(a)

        return carry

    lax.fori_loop(0, 10, one, 0)

    w_copies[4].wait()

    def take(d, c):
        red_wait(d)
        return c + buf3[d].astype(f32)

    def cand_rows():
        pl.when(p == 0)(lambda: red_wait(0))

        @pl.when(p == 1)
        def _():
            buf3[0] = out3[z, pl.ds(cr, cr)]

        cattn = lax.fori_loop(1, depth, take, buf3[0].astype(f32))
        return (layer_norm(cattn) * u_s[pl.ds(rows, cr)].astype(f32)).astype(bf16)

    def event_rows():
        return (layer_norm(acc[...]) * u_s[pl.ds(0, rows)].astype(f32)).astype(bf16)

    @pl.when(has_above)
    def _():
        out_ref[pl.ds(0, rows)] = (hist[...].astype(f32) + dot(event_rows(), w_out[...])).astype(bf16)

    for h in range(PIECES):
        for kind, src, dst, to, cond, _ in moves:
            if routed(kind, h):

                @pl.when(cond)
                def _():
                    x_copy(src, dst, h, kind, to).wait_send()

    for t, cond in ((0, (k == 0) | (p == 1)), (1, live(1)), (2, live(2)), (3, live(3) & (k == 1))):

        @pl.when(cond)
        def _():
            swap_copy(t).wait_send()

    @pl.when(live(3) & (k == 0))
    def _():
        swap_half(3).wait_send()
        swap_half(4).wait_send()

    pl.when(p == 0)(lambda: c_cross().wait_send())

    @pl.when(p == 1)
    def _():
        def left(d, c):
            pl.when(has_above & (z - d >= 0))(lambda: c_block(0, up_send.at[d], above).wait_send())
            pl.when(has_below & (z + d < depth))(lambda: c_block(0, down_send.at[d], below).wait_send())
            return c

        lax.fori_loop(0, depth, left, 0)

    @pl.when(has_above)
    def _():
        out_ref[pl.ds(rows, cr)] = (cand[...].astype(f32) + dot(cand_rows(), w_out[...])).astype(bf16)

    @pl.when(z + 1 == depth)
    def _():
        y_c = cand_rows()
        both = dot(jnp.concatenate([event_rows(), y_c], axis=0), w_out[...])
        out_ref[pl.ds(0, rows)] = (hist[...].astype(f32) + both[:rows]).astype(bf16)
        out_ref[pl.ds(rows, cr)] = (cand[...].astype(f32) + both[rows:]).astype(bf16)

    @pl.when(p == 1)
    def _():
        red(0, 0).wait_send()

        def sums(d, c):
            for side in range(2):
                red(d, side).wait_send()
            return c

        lax.fori_loop(1, depth, sums, 0)


def hand_out(both, out_ref, cout_ref, sem):
    rows, cr = out_ref.shape[0], cout_ref.shape[0]
    parts = (pl.ds(0, rows), pl.ds(rows, cr))
    to = (out_ref, cout_ref)
    saves = [pltpu.make_async_copy(both.at[at], to[i], sem.at[i]) for i, at in enumerate(parts)]
    for c in saves:
        c.start()
    for c in saves:
        c.wait()


def per_device(n, history, candidates, lengths, cand_user, w_in, w_out):
    rows, width = history.shape
    cr = candidates.shape[0]
    depth = n // ROW
    users = cand_user[None, :]
    vmem = pl.BlockSpec(memory_space=pltpu.VMEM)
    dma = pltpu.SemaphoreType.DMA
    block = depth * 2 * cr
    group = min(block, 256)
    both = pl.pallas_call(
        functools.partial(kernel, n),
        out_shape=jax.ShapeDtypeStruct((rows + cr, width), bf16),
        in_specs=[pl.BlockSpec(memory_space=pltpu.HBM)] * 6,
        out_specs=vmem,
        scratch_shapes=[
            pltpu.SMEM(lengths.shape, jnp.int32),
            pltpu.VMEM((rows, width), bf16),
            pltpu.VMEM((cr, width), bf16),
            pltpu.VMEM((1, cr), jnp.int32),
            dma((5,)),
            pltpu.VMEM((4, width, width), bf16),
            pltpu.VMEM((width, width), bf16),
            pltpu.VMEM((rows, width), bf16),
            pltpu.VMEM((5, rows, width), bf16),
            pltpu.VMEM((SIB + 5, 2, rows, width), bf16),
            pltpu.VMEM((rows, width), bf16),
            pltpu.VMEM((rows + cr, width), bf16),
            pltpu.VMEM((rows, width), f32),
            pltpu.VMEM((cr, width + 128), bf16),
            pltpu.VMEM((depth, 2 * cr, width + 128), bf16),
            pltpu.VMEM((group, width), bf16),
            pltpu.VMEM((block // group, group, width), f32),
            pltpu.VMEM((depth, 2 * cr, width), bf16),
            pltpu.VMEM((depth, cr, width), bf16),
            dma((5,)),
            dma((9, PIECES)),
            dma((5, PIECES)),
            dma((5,)),
            dma((5,)),
            dma((1,)),
            dma((depth + 1,)),
            dma((depth,)),
            dma((depth,)),
            dma((2, depth)),
            dma((depth,)),
        ],
        compiler_params=pltpu.CompilerParams(
            collective_id=0, has_side_effects=True, vmem_limit_bytes=52 * 1024 * 1024
        ),
    )(*(pltpu.with_memory_space_constraint(x, pltpu.HBM) for x in (lengths, history, candidates, users, w_in, w_out)))
    hbm = pl.BlockSpec(memory_space=pl.ANY)
    return pl.pallas_call(
        hand_out,
        out_shape=(
            jax.ShapeDtypeStruct((rows, width), bf16),
            jax.ShapeDtypeStruct((cr, width), bf16),
        ),
        in_specs=[vmem],
        out_specs=(hbm, hbm),
        scratch_shapes=[dma((2,))],
        compiler_params=pltpu.CompilerParams(vmem_limit_bytes=2 * 1024 * 1024),
    )(both)


def solution(mesh):
    n = mesh.shape["seq"]
    placed = (
        P(("grp", "seq"), None),
        P(("grp", "seq"), None),
        P("grp"),
        P(("grp", "seq")),
        P(),
        P(),
    )
    return jax.shard_map(
        functools.partial(per_device, n),
        mesh=mesh,
        in_specs=placed,
        out_specs=(P(("grp", "seq"), None), P(("grp", "seq"), None)),
        check_vma=False,
    )
```
